32 devices in a mesh: leaf: 8 (over z, y), sub: 4 (over x, core).
Axes of the slice: x: 2, y: 2, z: 4, core: 2. Of those that a mesh axis runs over, the one named last changes fastest.
Arguments:
- signal: bfloat16 [32, 65536], P(None, ('leaf', 'sub')), may hold values from -6 to 6
- row_basis: bfloat16 [64, 65536], P(None, ('leaf', 'sub')), may hold values from -0.375 to 0.375
- transfer: bfloat16 [512, 9, 32, 128], P(('leaf', 'sub')), may hold values from -0.5 to 0.5
- column_basis: bfloat16 [64, 65536], P(None, ('leaf', 'sub')), may hold values from -0.75 to 0.75
- near_blocks: bfloat16 [768, 128, 256], P(('leaf', 'sub')), may hold values from -0.375 to 0.375
- near_list: int32 [768, 2], P(('leaf', 'sub')), may hold values from -1 to 31, as said below
Outputs:
- result: float32 [32, 65536], P(None, ('leaf', 'sub'))
The draws below stay inside these ranges and needn't reach their ends.
Inputs may be any that keep to these rules, and one draw needn't show every extreme that they name: `near_list`: on each device the live entries (column >= 0) fill a leading run of its 24 slots, 2 or more of them, and empty slots hold -1 in both places; a live entry has 0 <= column < 24 and column <= row <= column + 8. Devices 2m and 2m + 1 hold at most 24 live entries together, and some such pair holds 24.
All inputs are finite; a program needn't handle non-finite values.
Results may differ from the reference program's by a relative error of at most 0.0003.
Values may be sent and summed in bfloat16 or wider, within the bound.
No kernel may reach another device: no remote copies, remote signals or barrier semaphores. Data moves between devices by JAX's collectives and lax.ppermute only.
A program may use at most 128 MiB of HBM per device.

```python
import jax
import jax.numpy as jnp
from jax import lax

BLOCK_RANK = 32
RHS = 16
LEAF = 128
BOX_DEV = 16
REACH = 4
CAP = 24
BUTTERFLY_DEPTH = 9
TOTAL_LEAF_BOXES = 512
NPTS = 65536
NEAR_SLOTS = 768
DEVICES = 32


def draw_near_list(key, part):
    pair_count = DEVICES // 2
    subkeys = jax.random.split(key, 6)
    heavy_count = jax.random.randint(subkeys[0], (pair_count,), CAP // 2, CAP - 1)
    full_pair = jax.random.randint(subkeys[1], (), 0, pair_count)
    heavy_count = jnp.where(jnp.arange(pair_count) == full_pair, CAP - 2, heavy_count)
    spare_room = CAP - heavy_count
    light_count = jax.random.randint(subkeys[2], (pair_count,), 2, spare_room + 1)
    heavy_first = jax.random.randint(subkeys[3], (pair_count,), 0, 2)
    first_count = jnp.where(heavy_first == 0, heavy_count, light_count)
    second_count = jnp.where(heavy_first == 0, light_count, heavy_count)
    counts = jnp.stack([first_count, second_count], axis=1).reshape(DEVICES)
    col_index = jax.random.randint(subkeys[4], (DEVICES, CAP), 0, BOX_DEV + 2 * REACH)
    offsets = jax.random.randint(subkeys[5], (DEVICES, CAP), 0, 2 * REACH + 1)
    slot_ids = jnp.arange(CAP)[None, :]
    col_index = jnp.where(slot_ids == 0, 0, col_index)
    offsets = jnp.where(slot_ids == 0, offsets % (2 * REACH), offsets)
    col_index = jnp.where(slot_ids == 1, BOX_DEV + 2 * REACH - 1, col_index)
    offsets = jnp.where(slot_ids == 1, 2 * REACH, offsets)
    row_index = col_index + offsets
    live_slot = slot_ids < counts[:, None]
    col_index = jnp.where(live_slot, col_index, -1)
    row_index = jnp.where(live_slot, row_index, -1)
    return jnp.stack([row_index, col_index], axis=-1).reshape(DEVICES * CAP, 2).astype(jnp.int32)


def shard_levels(own_key, extent, shards, smallest, high):
    def one(axis_at, parts):
        draws = jax.random.uniform(jax.random.fold_in(jax.random.fold_in(own_key, 6), axis_at), (parts,), jnp.float32, smallest / len(shards), high / len(shards))
        return jnp.repeat(jnp.exp(draws), extent[axis_at] // parts).reshape((-1,) + (1,) * (len(extent) - axis_at - 1))

    loudness = one(*shards[0])
    for cut in shards[1:]:
        loudness = loudness * one(*cut)
    return loudness


def gaussian(own_key, extent, deviation, reach, cuts=(), kind=jnp.bfloat16):
    level = shard_levels(own_key, extent, cuts, -0.22, 0.18) if cuts else 1.0
    drawn = jax.random.normal(own_key, extent, jnp.float32) * deviation * level
    return jnp.minimum(jnp.maximum(drawn, -reach), reach).astype(kind)


def setup_inputs(seed: int = 0) -> dict:
    streams_of = jax.random.split(jax.random.key(seed), 7)
    return {
        "signal": gaussian(streams_of[0], (2 * RHS, NPTS), 1.0, 6.0, ((1, 32),)),
        "row_basis": gaussian(streams_of[1], (2 * BLOCK_RANK, NPTS), (2 * LEAF) ** -0.5, 0.375, ((1, 32),)),
        "transfer": gaussian(streams_of[2], (TOTAL_LEAF_BOXES, BUTTERFLY_DEPTH, BLOCK_RANK, 4 * BLOCK_RANK), (4 * BLOCK_RANK) ** -0.5, 0.5, ((0, 32),)),
        "column_basis": gaussian(streams_of[3], (2 * BLOCK_RANK, NPTS), (2 * BLOCK_RANK) ** -0.5, 0.75, ((1, 32),)),
        "near_blocks": gaussian(streams_of[4], (NEAR_SLOTS, LEAF, 2 * LEAF), (2 * LEAF) ** -0.5, 0.375, ((0, 32),)),
        "near_list": draw_near_list(jax.random.fold_in(streams_of[6], 71), 0),
    }


highest = lax.Precision.HIGHEST


def project(signal, row_basis):
    rhs_count = signal.shape[0] // 2
    rank_width = row_basis.shape[0] // 2
    leaves = signal.shape[1] // LEAF
    samples = signal.astype(jnp.float32).reshape(2, rhs_count, leaves, LEAF)
    basis_rows = row_basis.astype(jnp.float32).reshape(2, rank_width, leaves, LEAF)
    products = jnp.einsum('xrlp,yqlp->xylrq', samples, basis_rows)
    real_part = products[0, 0] + products[1, 1]
    imag_part = products[1, 0] - products[0, 1]
    return jnp.transpose(jnp.concatenate([real_part, imag_part], axis=-1), (1, 0, 2))


def block_form(weights):
    matrices = weights.astype(jnp.float32)
    rank_width = matrices.shape[1]
    pieces = []
    for offspring in range(2):
        real_part = matrices[:, :, (2 * offspring) * rank_width:(2 * offspring + 1) * rank_width]
        imag_part = matrices[:, :, (2 * offspring + 1) * rank_width:(2 * offspring + 2) * rank_width]
        upper_rows = jnp.concatenate([real_part, -imag_part], axis=2)
        lower_rows = jnp.concatenate([imag_part, real_part], axis=2)
        pieces.append(jnp.concatenate([upper_rows, lower_rows], axis=1))
    return jnp.concatenate(pieces, axis=1)


def apply_level(paired, weights):
    return jnp.einsum('rsm,smn->rsn', paired, block_form(weights), precision=highest)


def pair_local(coeffs, height):
    rhs_count, slot_count, doubled = coeffs.shape
    half_span = 2 ** (height - 1)
    grouped = coeffs.reshape(rhs_count, slot_count // (2 * half_span), 2, half_span, doubled)
    joined = jnp.concatenate([grouped[:, :, 0], grouped[:, :, 1]], axis=-1)
    twice = jnp.stack([joined, joined], axis=2)
    return twice.reshape(rhs_count, slot_count, 2 * doubled)


def evaluate(coeffs, column_basis):
    rhs_count, leaves, doubled = coeffs.shape
    rank_width = doubled // 2
    basis_rows = column_basis.astype(jnp.float32).reshape(2, rank_width, leaves, LEAF)
    real_coefficient = coeffs[:, :, :rank_width]
    imag_coef = coeffs[:, :, rank_width:]
    real_out = (jnp.einsum('rlq,qlp->rlp', real_coefficient, basis_rows[0], precision=highest)
                - jnp.einsum('rlq,qlp->rlp', imag_coef, basis_rows[1], precision=highest))
    imag_out = (jnp.einsum('rlq,qlp->rlp', imag_coef, basis_rows[0], precision=highest)
                + jnp.einsum('rlq,qlp->rlp', real_coefficient, basis_rows[1], precision=highest))
    return jnp.concatenate([real_out, imag_out], axis=0).reshape(2 * rhs_count, leaves * LEAF)


def pick_rows(window, row_index):
    channels = window.shape[0]
    leaf_tiles = window.reshape(channels, -1, LEAF)
    picked = jnp.take(leaf_tiles, jnp.maximum(row_index, 0), axis=1)
    return jnp.transpose(picked, (1, 0, 2))


def near_products(picked, blocks):
    products = jnp.einsum('scp,spj->scj', picked.astype(jnp.float32), blocks.astype(jnp.float32))
    rhs_count = picked.shape[1] // 2
    real_part = products[:, :rhs_count, :LEAF] + products[:, rhs_count:, LEAF:]
    imag_part = products[:, rhs_count:, :LEAF] - products[:, :rhs_count, LEAF:]
    return jnp.concatenate([real_part, imag_part], axis=1)


def accumulate(output_values, col_index, box_count):
    selector = (col_index[:, None] == jnp.arange(box_count, dtype=jnp.int32)[None, :]).astype(jnp.float32)
    return jnp.einsum('sw,scj->cwj', selector, output_values, precision=highest)


def near_field(signal, near_blocks, near_list):
    channels = signal.shape[0]
    window_width = (BOX_DEV + 4 * REACH) * LEAF
    edge_width = 2 * REACH * LEAF
    extended = jnp.concatenate([signal[:, -edge_width:], signal, signal[:, :edge_width]], axis=1)
    blocks = near_blocks.reshape(DEVICES, CAP, LEAF, 2 * LEAF)
    entries = near_list.reshape(DEVICES, CAP, 2)

    def one_device(item_data):
        device, dev_blocks, dev_entries = item_data
        window = lax.dynamic_slice_in_dim(extended, device * (BOX_DEV * LEAF), window_width, 1)
        picked = pick_rows(window, dev_entries[:, 0])
        return accumulate(near_products(picked, dev_blocks), dev_entries[:, 1], BOX_DEV + 2 * REACH)

    windows = lax.map(one_device, (jnp.arange(DEVICES, dtype=jnp.int32), blocks, entries))
    center = windows[:, :, REACH:REACH + BOX_DEV]
    left_rim = windows[:, :, :REACH]
    right_rim = windows[:, :, BOX_DEV + REACH:]
    center = center.at[:, :, BOX_DEV - REACH:].add(jnp.roll(left_rim, -1, axis=0))
    center = center.at[:, :, :REACH].add(jnp.roll(right_rim, 1, axis=0))
    return jnp.transpose(center, (1, 0, 2, 3)).reshape(channels, DEVICES * BOX_DEV * LEAF)


def reference(signal, row_basis, transfer, column_basis, near_blocks, near_list):
    coeffs = project(signal, row_basis)
    for height in range(1, BUTTERFLY_DEPTH + 1):
        coeffs = apply_level(pair_local(coeffs, height), transfer[:, height - 1])
    far_field = evaluate(coeffs, column_basis)
    return far_field + near_field(signal, near_blocks, near_list)
```

```python
import functools

import jax
import jax.numpy as jnp
from jax import lax
from jax.experimental import pallas as pl
from jax.experimental.pallas import tpu as pltpu
from jax.sharding import PartitionSpec as P

LEAF = 128
AXES = ("leaf", "sub")
F32 = jnp.float32
BF16 = jnp.bfloat16


def lanes_like(x):
    return lax.broadcasted_iota(jnp.int32, x.shape, x.ndim - 1)


def dot(a, b):
    return lax.dot_general(a, b, (((1,), (0,)), ((), ())), preferred_element_type=F32)


def dot_t(a, b):
    return lax.dot_general(a, b, (((1,), (1,)), ((), ())), preferred_element_type=F32)


def half_roll(x):
    return pltpu.roll(x, x.shape[1] // 2, 1)


def pick_low(x, y):
    return jnp.where(lanes_like(x) < x.shape[1] // 2, x, y)


def split_rows(x):
    top = x.astype(BF16)
    rest = (x - top.astype(F32)).astype(BF16)
    return [top, rest]


def level_matrix(first, second):
    a = first.astype(F32)
    b = second.astype(F32)
    width = a.shape[1]
    quarter = width // 4
    low = pick_low(a, half_roll(b))
    high = pick_low(half_roll(a), b)
    is_real = lanes_like(a) % (2 * quarter) < quarter
    rows = []
    for part in (low, high):
        rows.append(jnp.where(is_real, part, -part))
        rows.append(jnp.where(is_real, pltpu.roll(part, width - quarter, 1), pltpu.roll(part, quarter, 1)))
    return jnp.concatenate(rows, axis=0).astype(BF16)


def project_pair(signal_ref, basis_ref, first, second):
    rhs = signal_ref.shape[0] // 2
    rank = basis_ref.shape[0] // 2
    left = []
    right = []
    for box in (first, second):
        cols = pl.ds(box * LEAF, LEAF)
        x = signal_ref[:, cols]
        u = basis_ref[:, cols]
        left.append(jnp.concatenate([x[:rhs], x[rhs:]], axis=1))
        right.append(jnp.concatenate([u[:rank], u[rank:]], axis=1))
        right.append(jnp.concatenate([-u[rank:], u[:rank]], axis=1))
    out = dot_t(jnp.concatenate(left, axis=0), jnp.concatenate(right, axis=0))
    return pick_low(out[:rhs], out[rhs:])


def local_kernel(signal_ref, basis_ref, transfer_ref, out_ref):
    boxes = transfer_ref.shape[0]
    rhs = signal_ref.shape[0] // 2
    levels = boxes.bit_length() - 1
    state = {}
    for box in range(0, boxes, 2):
        state[box] = project_pair(signal_ref, basis_ref, box, box + 1)
    for level in range(levels):
        bit = 1 << level
        done = {}
        for box, pair in state.items():
            matrix = level_matrix(transfer_ref[box, level], transfer_ref[box + bit, level])
            both = dot(jnp.concatenate(split_rows(pair), axis=0), matrix)
            done[box] = both[:rhs] + both[rhs:]
        state = done
        if level + 1 < levels:
            state = {}
            for box in done:
                if box & (2 * bit):
                    continue
                other = box + 2 * bit
                state[box] = pick_low(done[box], half_roll(done[other]))
                state[box + bit] = pick_low(half_roll(done[box]), done[other])
    for box, pair in state.items():
        out_ref[box] = pair


def matrices_kernel(transfer_ref, out_ref, *, first_level):
    half = transfer_ref.shape[0] // 2
    for level in range(out_ref.shape[0]):
        for box in range(half):
            out_ref[level, box] = level_matrix(
                transfer_ref[box, first_level + level], transfer_ref[box + half, first_level + level]
            )


def crossed(own_ref, other_ref, matrices_ref, level, upper, box):
    own = own_ref[box]
    other = other_ref[box]
    rhs = own.shape[0]
    low = jnp.where(upper, other, own)
    high = jnp.where(upper, own, other)
    first = pick_low(low, half_roll(high))
    second = pick_low(half_roll(low), high)
    rows = jnp.concatenate(split_rows(first) + split_rows(second), axis=0)
    out = dot(rows, matrices_ref[level, box])
    return pick_low(out[:rhs] + out[rhs : 2 * rhs], out[2 * rhs : 3 * rhs] + out[3 * rhs :])


def device_index():
    return lax.axis_index("leaf") * lax.axis_size("sub") + lax.axis_index("sub")


def cross_kernel(index_ref, own_ref, other_ref, matrices_ref, out_ref, *, level):
    upper = (index_ref[0] >> level & 1) == 1
    for box in range(own_ref.shape[0]):
        out_ref[box] = crossed(own_ref, other_ref, matrices_ref, level, upper, box)


def final_kernel(
    index_ref, own_ref, other_ref, matrices_ref, basis_ref, center_ref, pair_ref, ring_ref, out_ref, *, level
):
    upper = (index_ref[0] >> level & 1) == 1
    odd = (index_ref[0] & 1) == 1
    half, rhs, width = own_ref.shape
    rank = width // 4
    edge = pair_ref.shape[1] // LEAF
    for box in range(half):
        pair = crossed(own_ref, other_ref, matrices_ref, level, upper, box)
        is_low = lanes_like(pair) < width // 2
        rows = []
        for part in (jnp.where(is_low, pair, 0.0), jnp.where(is_low, 0.0, pair)):
            rows += split_rows(part)
        right = []
        for place in (box, box + half):
            v = basis_ref[:, pl.ds(place * LEAF, LEAF)]
            right.append(jnp.concatenate([v[:rank], v[rank:]], axis=1))
            right.append(jnp.concatenate([-v[rank:], v[:rank]], axis=1))
        out = dot(jnp.concatenate(rows, axis=0), jnp.concatenate(right, axis=0))
        for k, place in enumerate((box, box + half)):
            far = out[2 * k * rhs : (2 * k + 1) * rhs] + out[(2 * k + 1) * rhs : (2 * k + 2) * rhs]
            total = center_ref[place] + jnp.concatenate([far[:, :LEAF], far[:, LEAF:]], axis=0)
            if place < edge:
                cols = pl.ds(place * LEAF, LEAF)
                total = total + jnp.where(odd, pair_ref[:, cols], ring_ref[:, cols])
            if place >= 2 * half - edge:
                cols = pl.ds((place - 2 * half + edge) * LEAF, LEAF)
                total = total + jnp.where(odd, ring_ref[:, cols], pair_ref[:, cols])
            out_ref[:, pl.ds(place * LEAF, LEAF)] = total


def near_kernel(
    index_ref, list_ref, signal_ref, pair_ref, ring_ref, blocks_ref, center_ref, to_pair_ref, to_ring_ref, window, sums
):
    odd = (index_ref[0] & 1) == 1
    channels = signal_ref.shape[0]
    rhs = channels // 2
    boxes = signal_ref.shape[1] // LEAF
    halo = pair_ref.shape[1] // LEAF
    edge = to_pair_ref.shape[1] // LEAF
    for box in range(halo):
        cols = pl.ds(box * LEAF, LEAF)
        window[box] = jnp.where(odd, pair_ref[:, cols], ring_ref[:, cols])
        window[halo + boxes + box] = jnp.where(odd, ring_ref[:, cols], pair_ref[:, cols])
    for box in range(boxes):
        window[halo + box] = signal_ref[:, pl.ds(box * LEAF, LEAF)]
    sums[...] = jnp.zeros_like(sums)
    for slot in range(blocks_ref.shape[0]):
        row = jnp.maximum(list_ref[slot, 0], 0)
        col = list_ref[slot, 1]
        col = jnp.where(col < 0, sums.shape[0] - 1, col)
        out = dot(window[row], blocks_ref[slot])
        real = out[:rhs, :LEAF] + out[rhs:, LEAF:]
        imag = out[rhs:, :LEAF] - out[:rhs, LEAF:]
        sums[col] = sums[col] + jnp.concatenate([real, imag], axis=0)
    for box in range(boxes):
        center_ref[box] = sums[edge + box]
    for box in range(edge):
        cols = pl.ds(box * LEAF, LEAF)
        before = sums[box]
        after = sums[edge + boxes + box]
        to_pair_ref[:, cols] = jnp.where(odd, before, after)
        to_ring_ref[:, cols] = jnp.where(odd, after, before)


VMEM = pl.BlockSpec(memory_space=pltpu.VMEM)
SMEM = pl.BlockSpec(memory_space=pltpu.SMEM)


def shards(signal, row_basis, transfer, column_basis, near_blocks, near_list):
    channels = signal.shape[0]
    rhs = channels // 2
    boxes, levels, rank, width = transfer.shape
    half = boxes // 2
    reach = boxes // 4
    local_levels = boxes.bit_length() - 1
    devices = lax.axis_size("leaf") * lax.axis_size("sub")
    index = device_index()
    index_word = index.astype(jnp.int32).reshape(1)
    odd = index & 1

    pairs = [(i, i ^ 1) for i in range(devices)]
    ring = [(i, (i + 1) % devices if i & 1 else (i - 1) % devices) for i in range(devices)]

    halo = 2 * reach * LEAF
    far_end = signal.shape[1] - halo
    to_pair = lax.dynamic_slice_in_dim(signal, jnp.where(odd == 1, 0, far_end), halo, 1)
    to_ring = lax.dynamic_slice_in_dim(signal, jnp.where(odd == 1, far_end, 0), halo, 1)
    with jax.named_scope("halo_pair"):
        from_pair = lax.ppermute(to_pair, AXES, pairs)
    with jax.named_scope("halo_ring"):
        from_ring = lax.ppermute(to_ring, AXES, ring)

    state_type = jax.ShapeDtypeStruct((half, rhs, width), F32)
    coeffs = pl.pallas_call(
        local_kernel, out_shape=state_type, in_specs=[VMEM] * 3, out_specs=VMEM, name="local"
    )(signal, row_basis, transfer)
    cross_levels = levels - local_levels
    matrices = pl.pallas_call(
        functools.partial(matrices_kernel, first_level=local_levels),
        out_shape=jax.ShapeDtypeStruct((cross_levels, half, width, width), BF16),
        in_specs=[VMEM],
        out_specs=VMEM,
        name="matrices",
    )(transfer)
    center, rim_pair, rim_ring = pl.pallas_call(
        near_kernel,
        out_shape=(
            jax.ShapeDtypeStruct((boxes, channels, LEAF), F32),
            jax.ShapeDtypeStruct((channels, reach * LEAF), F32),
            jax.ShapeDtypeStruct((channels, reach * LEAF), F32),
        ),
        in_specs=[SMEM, SMEM, VMEM, VMEM, VMEM, VMEM],
        out_specs=(VMEM, VMEM, VMEM),
        scratch_shapes=[
            pltpu.VMEM((boxes + 4 * reach, channels, LEAF), BF16),
            pltpu.VMEM((boxes + 2 * reach + 1, channels, LEAF), F32),
        ],
        name="near",
    )(index_word, near_list, signal, from_pair, from_ring, near_blocks)
    with jax.named_scope("rim_pair"):
        rim_from_pair = lax.ppermute(rim_pair, AXES, pairs)
    with jax.named_scope("rim_ring"):
        rim_from_ring = lax.ppermute(rim_ring, AXES, ring)

    for level in range(cross_levels):
        with jax.named_scope(f"swap_{level}"):
            other = lax.ppermute(coeffs, AXES, [(i, i ^ 1 << level) for i in range(devices)])
        if level + 1 < cross_levels:
            coeffs = pl.pallas_call(
                functools.partial(cross_kernel, level=level),
                out_shape=state_type,
                in_specs=[SMEM, VMEM, VMEM, VMEM],
                out_specs=VMEM,
                name=f"cross_{level}",
            )(index_word, coeffs, other, matrices)
    return pl.pallas_call(
        functools.partial(final_kernel, level=cross_levels - 1),
        out_shape=jax.ShapeDtypeStruct((channels, boxes * LEAF), F32),
        in_specs=[SMEM] + [VMEM] * 7,
        out_specs=VMEM,
        name="final",
    )(index_word, coeffs, other, matrices, column_basis, center, rim_from_pair, rim_from_ring)


def solution(mesh):
    return jax.shard_map(
        shards,
        mesh=mesh,
        in_specs=(
            P(None, AXES),
            P(None, AXES),
            P(AXES, None, None, None),
            P(None, AXES),
            P(AXES, None, None),
            P(AXES, None),
        ),
        out_specs=P(None, AXES),
        check_vma=False,
    )
```

```python
import functools

import jax
import jax.numpy as jnp
from jax import lax
from jax.experimental import pallas as pl
from jax.experimental.pallas import tpu as pltpu
from jax.sharding import PartitionSpec as P

LEAF = 128
AXES = ("leaf", "sub")
F32 = jnp.float32
BF16 = jnp.bfloat16


def lanes_like(x):
    return lax.broadcasted_iota(jnp.int32, x.shape, x.ndim - 1)


def dot(a, b):
    return lax.dot_general(a, b, (((1,), (0,)), ((), ())), preferred_element_type=F32)


def dot_t(a, b):
    return lax.dot_general(a, b, (((1,), (1,)), ((), ())), preferred_element_type=F32)


def half_roll(x):
    return pltpu.roll(x, x.shape[1] // 2, 1)


def pick_low(x, y):
    return jnp.where(lanes_like(x) < x.shape[1] // 2, x, y)


def split_rows(x):
    top = x.astype(BF16)
    rest = (x - top.astype(F32)).astype(BF16)
    return [top, rest]


def level_matrix(first, second):
    a = first.astype(F32)
    b = second.astype(F32)
    width = a.shape[1]
    quarter = width // 4
    low = pick_low(a, half_roll(b))
    high = pick_low(half_roll(a), b)
    is_real = lanes_like(a) % (2 * quarter) < quarter
    rows = []
    for part in (low, high):
        rows.append(jnp.where(is_real, part, -part))
        rows.append(jnp.where(is_real, pltpu.roll(part, width - quarter, 1), pltpu.roll(part, quarter, 1)))
    return jnp.concatenate(rows, axis=0).astype(BF16)


def project_pair(signal_ref, basis_ref, first, second):
    rhs = signal_ref.shape[0] // 2
    rank = basis_ref.shape[0] // 2
    left = []
    right = []
    for box in (first, second):
        cols = pl.ds(box * LEAF, LEAF)
        x = signal_ref[:, cols]
        u = basis_ref[:, cols]
        left.append(jnp.concatenate([x[:rhs], x[rhs:]], axis=1))
        right.append(jnp.concatenate([u[:rank], u[rank:]], axis=1))
        right.append(jnp.concatenate([-u[rank:], u[:rank]], axis=1))
    out = dot_t(jnp.concatenate(left, axis=0), jnp.concatenate(right, axis=0))
    return pick_low(out[:rhs], out[rhs:])


def local_kernel(signal_ref, basis_ref, transfer_ref, out_ref):
    boxes = transfer_ref.shape[0]
    rhs = signal_ref.shape[0] // 2
    levels = boxes.bit_length() - 1
    state = {}
    for box in range(0, boxes, 2):
        state[box] = project_pair(signal_ref, basis_ref, box, box + 1)
    for level in range(levels):
        bit = 1 << level
        done = {}
        for box, pair in state.items():
            matrix = level_matrix(transfer_ref[box, level], transfer_ref[box + bit, level])
            both = dot(jnp.concatenate(split_rows(pair), axis=0), matrix)
            done[box] = both[:rhs] + both[rhs:]
        state = done
        if level + 1 < levels:
            state = {}
            for box in done:
                if box & (2 * bit):
                    continue
                other = box + 2 * bit
                state[box] = pick_low(done[box], half_roll(done[other]))
                state[box + bit] = pick_low(half_roll(done[box]), done[other])
    for box, pair in state.items():
        out_ref[box] = pair


def matrices_kernel(transfer_ref, out_ref, *, first_level):
    half = transfer_ref.shape[0] // 2
    for level in range(out_ref.shape[0]):
        for box in range(half):
            out_ref[level, box] = level_matrix(
                transfer_ref[box, first_level + level], transfer_ref[box + half, first_level + level]
            )


def crossed(own_ref, other_ref, matrices_ref, level, upper, box):
    own = own_ref[box]
    other = other_ref[box]
    rhs = own.shape[0]
    low = jnp.where(upper, other, own)
    high = jnp.where(upper, own, other)
    first = pick_low(low, half_roll(high))
    second = pick_low(half_roll(low), high)
    rows = jnp.concatenate(split_rows(first) + split_rows(second), axis=0)
    out = dot(rows, matrices_ref[level, box])
    return pick_low(out[:rhs] + out[rhs : 2 * rhs], out[2 * rhs : 3 * rhs] + out[3 * rhs :])


def device_index():
    return lax.axis_index("leaf") * lax.axis_size("sub") + lax.axis_index("sub")


def cross_kernel(index_ref, own_ref, other_ref, matrices_ref, out_ref, *, level):
    upper = (index_ref[0] >> level & 1) == 1
    for box in range(own_ref.shape[0]):
        out_ref[box] = crossed(own_ref, other_ref, matrices_ref, level, upper, box)


def final_kernel(
    index_ref, own_ref, other_ref, matrices_ref, basis_ref, center_ref, pair_ref, ring_ref, out_ref, *, level
):
    upper = (index_ref[0] >> level & 1) == 1
    odd = (index_ref[0] & 1) == 1
    half, rhs, width = own_ref.shape
    rank = width // 4
    edge = pair_ref.shape[1] // LEAF
    for box in range(half):
        pair = crossed(own_ref, other_ref, matrices_ref, level, upper, box)
        is_low = lanes_like(pair) < width // 2
        rows = []
        for part in (jnp.where(is_low, pair, 0.0), jnp.where(is_low, 0.0, pair)):
            rows += split_rows(part)
        right = []
        for place in (box, box + half):
            v = basis_ref[:, pl.ds(place * LEAF, LEAF)]
            right.append(jnp.concatenate([v[:rank], v[rank:]], axis=1))
            right.append(jnp.concatenate([-v[rank:], v[:rank]], axis=1))
        out = dot(jnp.concatenate(rows, axis=0), jnp.concatenate(right, axis=0))
        for k, place in enumerate((box, box + half)):
            far = out[2 * k * rhs : (2 * k + 1) * rhs] + out[(2 * k + 1) * rhs : (2 * k + 2) * rhs]
            total = center_ref[place] + jnp.concatenate([far[:, :LEAF], far[:, LEAF:]], axis=0)
            if place < edge:
                cols = pl.ds(place * LEAF, LEAF)
                total = total + jnp.where(odd, pair_ref[:, cols], ring_ref[:, cols])
            if place >= 2 * half - edge:
                cols = pl.ds((place - 2 * half + edge) * LEAF, LEAF)
                total = total + jnp.where(odd, ring_ref[:, cols], pair_ref[:, cols])
            out_ref[:, pl.ds(place * LEAF, LEAF)] = total


def near_kernel(
    index_ref, list_ref, signal_ref, pair_ref, ring_ref, blocks_ref, center_ref, to_pair_ref, to_ring_ref, window, sums
):
    odd = (index_ref[0] & 1) == 1
    channels = signal_ref.shape[0]
    rhs = channels // 2
    boxes = signal_ref.shape[1] // LEAF
    halo = pair_ref.shape[1] // LEAF
    edge = to_pair_ref.shape[1] // LEAF
    for box in range(halo):
        cols = pl.ds(box * LEAF, LEAF)
        window[box] = jnp.where(odd, pair_ref[:, cols], ring_ref[:, cols])
        window[halo + boxes + box] = jnp.where(odd, ring_ref[:, cols], pair_ref[:, cols])
    for box in range(boxes):
        window[halo + box] = signal_ref[:, pl.ds(box * LEAF, LEAF)]
    sums[...] = jnp.zeros_like(sums)
    for slot in range(blocks_ref.shape[0]):
        row = jnp.maximum(list_ref[0, slot], 0)
        col = list_ref[1, slot]
        col = jnp.where(col < 0, sums.shape[0] - 1, col)
        out = dot(window[row], blocks_ref[slot])
        real = out[:rhs, :LEAF] + out[rhs:, LEAF:]
        imag = out[rhs:, :LEAF] - out[:rhs, LEAF:]
        sums[col] = sums[col] + jnp.concatenate([real, imag], axis=0)
    for box in range(boxes):
        center_ref[box] = sums[edge + box]
    for box in range(edge):
        cols = pl.ds(box * LEAF, LEAF)
        before = sums[box]
        after = sums[edge + boxes + box]
        to_pair_ref[:, cols] = jnp.where(odd, before, after)
        to_ring_ref[:, cols] = jnp.where(odd, after, before)


VMEM = pl.BlockSpec(memory_space=pltpu.VMEM)
SMEM = pl.BlockSpec(memory_space=pltpu.SMEM)


def on_chip(kernel, name, outs, scalars, arrays, scratch=(), grant=16 << 20):
    single = len(outs) == 2 and not isinstance(outs[1], tuple)
    shapes = tuple(pltpu.VMEM(shape, kind) for shape, kind in ((outs,) if single else outs))
    call = pl.pallas_call(
        kernel,
        out_shape=shapes[0] if single else shapes,
        in_specs=[SMEM] * len(scalars) + [VMEM] * len(arrays),
        out_specs=VMEM if single else (VMEM,) * len(shapes),
        scratch_shapes=list(scratch),
        compiler_params=pltpu.CompilerParams(vmem_limit_bytes=grant),
        name=name,
    )
    return call(*scalars, *[pltpu.with_memory_space_constraint(x, pltpu.VMEM) for x in arrays])


def shards(signal, row_basis, transfer, column_basis, near_blocks, near_list):
    channels = signal.shape[0]
    rhs = channels // 2
    boxes, levels, rank, width = transfer.shape
    half = boxes // 2
    reach = boxes // 4
    local_levels = boxes.bit_length() - 1
    devices = lax.axis_size("leaf") * lax.axis_size("sub")
    index = device_index()
    index_word = index.astype(jnp.int32).reshape(1)
    odd = index & 1

    pairs = [(i, i ^ 1) for i in range(devices)]
    ring = [(i, (i + 1) % devices if i & 1 else (i - 1) % devices) for i in range(devices)]

    halo = 2 * reach * LEAF
    far_end = signal.shape[1] - halo
    to_pair = lax.dynamic_slice_in_dim(signal, jnp.where(odd == 1, 0, far_end), halo, 1)
    to_ring = lax.dynamic_slice_in_dim(signal, jnp.where(odd == 1, far_end, 0), halo, 1)
    with jax.named_scope("halo_pair"):
        from_pair = lax.ppermute(to_pair, AXES, pairs)
    with jax.named_scope("halo_ring"):
        from_ring = lax.ppermute(to_ring, AXES, ring)

    state = ((half, rhs, width), F32)
    coeffs = on_chip(local_kernel, "local", state, (), (signal, row_basis, transfer))
    cross_levels = levels - local_levels
    matrices = on_chip(
        functools.partial(matrices_kernel, first_level=local_levels),
        "matrices",
        ((cross_levels, half, width, width), BF16),
        (),
        (transfer,),
    )
    center, rim_pair, rim_ring = on_chip(
        near_kernel,
        "near",
        (
            ((boxes, channels, LEAF), F32),
            ((channels, reach * LEAF), F32),
            ((channels, reach * LEAF), F32),
        ),
        (index_word, near_list.T),
        (signal, from_pair, from_ring, near_blocks),
        scratch=(
            pltpu.VMEM((boxes + 4 * reach, channels, LEAF), BF16),
            pltpu.VMEM((boxes + 2 * reach + 1, channels, LEAF), F32),
        ),
    )
    with jax.named_scope("rim_pair"):
        rim_from_pair = lax.ppermute(rim_pair, AXES, pairs)
    with jax.named_scope("rim_ring"):
        rim_from_ring = lax.ppermute(rim_ring, AXES, ring)

    for level in range(cross_levels):
        with jax.named_scope(f"swap_{level}"):
            other = lax.ppermute(coeffs, AXES, [(i, i ^ 1 << level) for i in range(devices)])
        if level + 1 < cross_levels:
            coeffs = on_chip(
                functools.partial(cross_kernel, level=level),
                f"cross_{level}",
                state,
                (index_word,),
                (coeffs, other, matrices),
            )
    return pl.pallas_call(
        functools.partial(final_kernel, level=cross_levels - 1),
        out_shape=jax.ShapeDtypeStruct((channels, boxes * LEAF), F32),
        in_specs=[SMEM] + [VMEM] * 7,
        out_specs=VMEM,
        compiler_params=pltpu.CompilerParams(vmem_limit_bytes=16 << 20),
        name="final",
    )(
        index_word,
        *[
            pltpu.with_memory_space_constraint(x, pltpu.VMEM)
            for x in (coeffs, other, matrices, column_basis, center, rim_from_pair, rim_from_ring)
        ],
    )


def solution(mesh):
    return jax.shard_map(
        shards,
        mesh=mesh,
        in_specs=(
            P(None, AXES),
            P(None, AXES),
            P(AXES, None, None, None),
            P(None, AXES),
            P(AXES, None, None),
            P(AXES, None),
        ),
        out_specs=P(None, AXES),
        check_vma=False,
    )
```

```python
import functools

import jax
import jax.numpy as jnp
import numpy as np
from jax import lax
from jax.experimental import pallas as pl
from jax.experimental.pallas import tpu as pltpu
from jax.sharding import PartitionSpec as P

LEAF = 128
AXES = ("leaf", "sub")
F32 = jnp.float32
BF16 = jnp.bfloat16


def lanes_like(x):
    return lax.broadcasted_iota(jnp.int32, x.shape, x.ndim - 1)


def dot(a, b):
    return lax.dot_general(a, b, (((1,), (0,)), ((), ())), preferred_element_type=F32)


def dot_t(a, b):
    return lax.dot_general(a, b, (((1,), (1,)), ((), ())), preferred_element_type=F32)


def half_roll(x):
    return pltpu.roll(x, x.shape[1] // 2, 1)


def pick_low(x, y):
    return jnp.where(lanes_like(x) < x.shape[1] // 2, x, y)


def split_rows(x):
    top = x.astype(BF16)
    rest = (x - top.astype(F32)).astype(BF16)
    return [top, rest]


def form_table(rank):
    width = 4 * rank
    table = np.zeros((2 * width, 4 * width), np.float32)
    unit = np.eye(rank, dtype=np.float32)
    for group in range(4):
        child, imag = divmod(group, 2)
        for box in range(2):
            for part in range(2):
                source = box * width + child * 2 * rank + (part ^ imag) * rank
                target = group * width + box * 2 * rank + part * rank
                sign = -1.0 if part and not imag else 1.0
                table[source : source + rank, target : target + rank] = sign * unit
    return table


def level_matrices(blocks, pairs, table):
    rows = [jnp.concatenate([blocks[first], blocks[second]], axis=1) for first, second in pairs]
    rank, width = rows[0].shape
    width //= 2
    out = dot(jnp.concatenate(rows, axis=0), table).astype(BF16)
    return [
        jnp.concatenate(
            [out[k * rank : (k + 1) * rank, g * width : (g + 1) * width] for g in range(4)], axis=0
        )
        for k in range(len(pairs))
    ]


def project_pair(signal_ref, basis_ref, first, second):
    rhs = signal_ref.shape[0] // 2
    rank = basis_ref.shape[0] // 2
    left = []
    right = []
    for box in (first, second):
        cols = pl.ds(box * LEAF, LEAF)
        x = signal_ref[:, cols]
        u = basis_ref[:, cols]
        left.append(jnp.concatenate([x[:rhs], x[rhs:]], axis=1))
        right.append(jnp.concatenate([u[:rank], u[rank:]], axis=1))
        right.append(jnp.concatenate([-u[rank:], u[:rank]], axis=1))
    out = dot_t(jnp.concatenate(left, axis=0), jnp.concatenate(right, axis=0))
    return pick_low(out[:rhs], out[rhs:])


def local_kernel(
    signal_hbm, basis_hbm, transfer_hbm, table_hbm, out_ref, signal_ref, basis_ref, transfer_ref, table_ref, arrived
):
    boxes, levels = transfer_ref.shape[:2]
    rhs = signal_ref.shape[0] // 2
    copies = [
        pltpu.make_async_copy(signal_hbm, signal_ref, arrived.at[0]),
        pltpu.make_async_copy(basis_hbm, basis_ref, arrived.at[1]),
        pltpu.make_async_copy(table_hbm, table_ref, arrived.at[2]),
        pltpu.make_async_copy(transfer_hbm.at[:, pl.ds(0, levels)], transfer_ref, arrived.at[3]),
    ]
    for copy in copies:
        copy.start()
    for copy in copies[:2]:
        copy.wait()
    state = {}
    for box in range(0, boxes, 2):
        state[box] = project_pair(signal_ref, basis_ref, box, box + 1)
    for copy in copies[2:]:
        copy.wait()
    table = table_ref[...]
    for level in range(levels):
        bit = 1 << level
        blocks = [transfer_ref[box, level] for box in range(boxes)]
        matrices = level_matrices(blocks, [(box, box + bit) for box in state], table)
        done = {}
        for matrix, (box, pair) in zip(matrices, state.items()):
            both = dot(jnp.concatenate(split_rows(pair), axis=0), matrix)
            done[box] = both[:rhs] + both[rhs:]
        state = done
        if level + 1 < levels:
            state = {}
            for box in done:
                if box & (2 * bit):
                    continue
                other = box + 2 * bit
                state[box] = pick_low(done[box], half_roll(done[other]))
                state[box + bit] = pick_low(half_roll(done[box]), done[other])
    for box, pair in state.items():
        out_ref[box] = pair


def matrices_kernel(transfer_ref, table_ref, out_ref, *, first_level):
    boxes = transfer_ref.shape[0]
    half = boxes // 2
    table = table_ref[...]
    for level in range(out_ref.shape[0]):
        blocks = [transfer_ref[box, first_level + level] for box in range(boxes)]
        matrices = level_matrices(blocks, [(box, box + half) for box in range(half)], table)
        for box in range(half):
            out_ref[level, box] = matrices[box]


def crossed(own_ref, other_ref, matrices_ref, level, upper, box):
    own = own_ref[box]
    other = other_ref[box]
    rhs = own.shape[0]
    low = jnp.where(upper, other, own)
    high = jnp.where(upper, own, other)
    first = pick_low(low, half_roll(high))
    second = pick_low(half_roll(low), high)
    rows = jnp.concatenate(split_rows(first) + split_rows(second), axis=0)
    out = dot(rows, matrices_ref[level, box])
    return pick_low(out[:rhs] + out[rhs : 2 * rhs], out[2 * rhs : 3 * rhs] + out[3 * rhs :])


def device_index():
    return lax.axis_index("leaf") * lax.axis_size("sub") + lax.axis_index("sub")


def cross_kernel(index_ref, own_ref, other_ref, matrices_ref, out_ref, *, level):
    upper = (index_ref[0] >> level & 1) == 1
    for box in range(own_ref.shape[0]):
        out_ref[box] = crossed(own_ref, other_ref, matrices_ref, level, upper, box)


def final_kernel(
    index_ref, own_ref, other_ref, matrices_ref, basis_ref, center_ref, pair_ref, ring_ref, out_ref, *, level
):
    upper = (index_ref[0] >> level & 1) == 1
    odd = (index_ref[0] & 1) == 1
    half, rhs, width = own_ref.shape
    rank = width // 4
    edge = pair_ref.shape[1] // LEAF
    for box in range(half):
        pair = crossed(own_ref, other_ref, matrices_ref, level, upper, box)
        is_low = lanes_like(pair) < width // 2
        rows = []
        for part in (jnp.where(is_low, pair, 0.0), jnp.where(is_low, 0.0, pair)):
            rows += split_rows(part)
        right = []
        for place in (box, box + half):
            v = basis_ref[:, pl.ds(place * LEAF, LEAF)]
            right.append(jnp.concatenate([v[:rank], v[rank:]], axis=1))
            right.append(jnp.concatenate([-v[rank:], v[:rank]], axis=1))
        out = dot(jnp.concatenate(rows, axis=0), jnp.concatenate(right, axis=0))
        for k, place in enumerate((box, box + half)):
            far = out[2 * k * rhs : (2 * k + 1) * rhs] + out[(2 * k + 1) * rhs : (2 * k + 2) * rhs]
            total = center_ref[place] + jnp.concatenate([far[:, :LEAF], far[:, LEAF:]], axis=0)
            if place < edge:
                cols = pl.ds(place * LEAF, LEAF)
                total = total + jnp.where(odd, pair_ref[:, cols], ring_ref[:, cols])
            if place >= 2 * half - edge:
                cols = pl.ds((place - 2 * half + edge) * LEAF, LEAF)
                total = total + jnp.where(odd, ring_ref[:, cols], pair_ref[:, cols])
            out_ref[:, pl.ds(place * LEAF, LEAF)] = total


def near_kernel(
    index_ref, list_ref, signal_ref, pair_ref, ring_ref, blocks_ref, center_ref, to_pair_ref, to_ring_ref, window, sums
):
    odd = (index_ref[0] & 1) == 1
    channels = signal_ref.shape[0]
    rhs = channels // 2
    boxes = signal_ref.shape[1] // LEAF
    halo = pair_ref.shape[1] // LEAF
    edge = to_pair_ref.shape[1] // LEAF
    for box in range(halo):
        cols = pl.ds(box * LEAF, LEAF)
        window[box] = jnp.where(odd, pair_ref[:, cols], ring_ref[:, cols])
        window[halo + boxes + box] = jnp.where(odd, ring_ref[:, cols], pair_ref[:, cols])
    for box in range(boxes):
        window[halo + box] = signal_ref[:, pl.ds(box * LEAF, LEAF)]
    sums[...] = jnp.zeros_like(sums)
    for slot in range(blocks_ref.shape[0]):
        row = jnp.maximum(list_ref[0, slot], 0)
        col = list_ref[1, slot]
        col = jnp.where(col < 0, sums.shape[0] - 1, col)
        out = dot(window[row], blocks_ref[slot])
        real = out[:rhs, :LEAF] + out[rhs:, LEAF:]
        imag = out[rhs:, :LEAF] - out[:rhs, LEAF:]
        sums[col] = sums[col] + jnp.concatenate([real, imag], axis=0)
    for box in range(boxes):
        center_ref[box] = sums[edge + box]
    for box in range(edge):
        cols = pl.ds(box * LEAF, LEAF)
        before = sums[box]
        after = sums[edge + boxes + box]
        to_pair_ref[:, cols] = jnp.where(odd, before, after)
        to_ring_ref[:, cols] = jnp.where(odd, after, before)


VMEM = pl.BlockSpec(memory_space=pltpu.VMEM)
SMEM = pl.BlockSpec(memory_space=pltpu.SMEM)


def on_chip(kernel, name, outs, scalars, arrays, scratch=(), grant=16 << 20):
    single = len(outs) == 2 and not isinstance(outs[1], tuple)
    shapes = tuple(pltpu.VMEM(shape, kind) for shape, kind in ((outs,) if single else outs))
    call = pl.pallas_call(
        kernel,
        out_shape=shapes[0] if single else shapes,
        in_specs=[SMEM] * len(scalars) + [VMEM] * len(arrays),
        out_specs=VMEM if single else (VMEM,) * len(shapes),
        scratch_shapes=list(scratch),
        compiler_params=pltpu.CompilerParams(vmem_limit_bytes=grant),
        name=name,
    )
    return call(*scalars, *[pltpu.with_memory_space_constraint(x, pltpu.VMEM) for x in arrays])


def shards(signal, row_basis, transfer, column_basis, near_blocks, near_list):
    channels = signal.shape[0]
    rhs = channels // 2
    boxes, levels, rank, width = transfer.shape
    half = boxes // 2
    reach = boxes // 4
    local_levels = boxes.bit_length() - 1
    devices = lax.axis_size("leaf") * lax.axis_size("sub")
    index = device_index()
    index_word = index.astype(jnp.int32).reshape(1)
    odd = index & 1

    pairs = [(i, i ^ 1) for i in range(devices)]
    ring = [(i, (i + 1) % devices if i & 1 else (i - 1) % devices) for i in range(devices)]

    halo = 2 * reach * LEAF
    far_end = signal.shape[1] - halo
    to_pair = lax.dynamic_slice_in_dim(signal, jnp.where(odd == 1, 0, far_end), halo, 1)
    to_ring = lax.dynamic_slice_in_dim(signal, jnp.where(odd == 1, far_end, 0), halo, 1)
    with jax.named_scope("halo_pair"):
        from_pair = lax.ppermute(to_pair, AXES, pairs)
    with jax.named_scope("halo_ring"):
        from_ring = lax.ppermute(to_ring, AXES, ring)

    table = jnp.asarray(form_table(rank), BF16)
    state = ((half, rhs, width), F32)
    coeffs = pl.pallas_call(
        local_kernel,
        out_shape=pltpu.VMEM(*state),
        in_specs=[pl.BlockSpec(memory_space=pl.ANY)] * 4,
        out_specs=VMEM,
        scratch_shapes=[
            pltpu.VMEM(signal.shape, BF16),
            pltpu.VMEM(row_basis.shape, BF16),
            pltpu.VMEM((boxes, local_levels, rank, width), BF16),
            pltpu.VMEM(table.shape, BF16),
            pltpu.SemaphoreType.DMA((4,)),
        ],
        compiler_params=pltpu.CompilerParams(vmem_limit_bytes=16 << 20),
        name="local",
    )(*[pltpu.with_memory_space_constraint(x, pltpu.HBM) for x in (signal, row_basis, transfer, table)])
    cross_levels = levels - local_levels
    matrices = on_chip(
        functools.partial(matrices_kernel, first_level=local_levels),
        "matrices",
        ((cross_levels, half, width, width), BF16),
        (),
        (transfer, table),
    )
    center, rim_pair, rim_ring = on_chip(
        near_kernel,
        "near",
        (
            ((boxes, channels, LEAF), F32),
            ((channels, reach * LEAF), F32),
            ((channels, reach * LEAF), F32),
        ),
        (index_word, near_list.T),
        (signal, from_pair, from_ring, near_blocks),
        scratch=(
            pltpu.VMEM((boxes + 4 * reach, channels, LEAF), BF16),
            pltpu.VMEM((boxes + 2 * reach + 1, channels, LEAF), F32),
        ),
    )
    with jax.named_scope("rim_pair"):
        rim_from_pair = lax.ppermute(rim_pair, AXES, pairs)
    with jax.named_scope("rim_ring"):
        rim_from_ring = lax.ppermute(rim_ring, AXES, ring)

    for level in range(cross_levels):
        with jax.named_scope(f"swap_{level}"):
            other = lax.ppermute(coeffs, AXES, [(i, i ^ 1 << level) for i in range(devices)])
        if level + 1 < cross_levels:
            coeffs = on_chip(
                functools.partial(cross_kernel, level=level),
                f"cross_{level}",
                state,
                (index_word,),
                (coeffs, other, matrices),
            )
    return pl.pallas_call(
        functools.partial(final_kernel, level=cross_levels - 1),
        out_shape=jax.ShapeDtypeStruct((channels, boxes * LEAF), F32),
        in_specs=[SMEM] + [VMEM] * 7,
        out_specs=VMEM,
        compiler_params=pltpu.CompilerParams(vmem_limit_bytes=16 << 20),
        name="final",
    )(
        index_word,
        *[
            pltpu.with_memory_space_constraint(x, pltpu.VMEM)
            for x in (coeffs, other, matrices, column_basis, center, rim_from_pair, rim_from_ring)
        ],
    )


def solution(mesh):
    return jax.shard_map(
        shards,
        mesh=mesh,
        in_specs=(
            P(None, AXES),
            P(None, AXES),
            P(AXES, None, None, None),
            P(None, AXES),
            P(AXES, None, None),
            P(AXES, None),
        ),
        out_specs=P(None, AXES),
        check_vma=False,
    )
```

```python
import functools

import jax
import jax.numpy as jnp
import numpy as np
from jax import lax
from jax.experimental import pallas as pl
from jax.experimental.pallas import tpu as pltpu
from jax.sharding import PartitionSpec as P


LEAF = 128
AXES = ("leaf", "sub")
F32 = jnp.float32
BF16 = jnp.bfloat16


def lanes_like(x):
    return lax.broadcasted_iota(jnp.int32, x.shape, x.ndim - 1)


def dot(a, b):
    return lax.dot_general(a, b, (((1,), (0,)), ((), ())), preferred_element_type=F32)


def dot_t(a, b):
    return lax.dot_general(a, b, (((1,), (1,)), ((), ())), preferred_element_type=F32)


def half_roll(x):
    return pltpu.roll(x, x.shape[1] // 2, 1)


def pick_low(x, y):
    return jnp.where(lanes_like(x) < x.shape[1] // 2, x, y)


def split_rows(x):
    top = x.astype(BF16)
    rest = (x - top.astype(F32)).astype(BF16)
    return [top, rest]


def form_table(rank):
    width = 4 * rank
    table = np.zeros((2 * width, 4 * width), np.float32)
    unit = np.eye(rank, dtype=np.float32)
    for group in range(4):
        child, imag = divmod(group, 2)
        for box in range(2):
            for part in range(2):
                source = box * width + child * 2 * rank + (part ^ imag) * rank
                target = group * width + box * 2 * rank + part * rank
                sign = -1.0 if part and not imag else 1.0
                table[source : source + rank, target : target + rank] = sign * unit
    return table


def level_matrices(blocks, pairs, table):
    rows = [jnp.concatenate([blocks[first], blocks[second]], axis=1) for first, second in pairs]
    rank, width = rows[0].shape
    width //= 2
    out = dot(jnp.concatenate(rows, axis=0), table).astype(BF16)
    return [
        jnp.concatenate(
            [out[k * rank : (k + 1) * rank, g * width : (g + 1) * width] for g in range(4)], axis=0
        )
        for k in range(len(pairs))
    ]


def project_pair(signal_ref, basis_ref, first, second):
    rhs = signal_ref.shape[0] // 2
    rank = basis_ref.shape[0] // 2
    left = []
    right = []
    for box in (first, second):
        cols = pl.ds(box * LEAF, LEAF)
        x = signal_ref[:, cols]
        u = basis_ref[:, cols]
        left.append(jnp.concatenate([x[:rhs], x[rhs:]], axis=1))
        right.append(jnp.concatenate([u[:rank], u[rank:]], axis=1))
        right.append(jnp.concatenate([-u[rank:], u[:rank]], axis=1))
    out = dot_t(jnp.concatenate(left, axis=0), jnp.concatenate(right, axis=0))
    return pick_low(out[:rhs], out[rhs:])


def local_kernel(
    signal_hbm, basis_hbm, transfer_hbm, table_hbm, out_ref, signal_ref, basis_ref, transfer_ref, table_ref, arrived
):
    boxes, levels = transfer_ref.shape[:2]
    rhs = signal_ref.shape[0] // 2
    copies = [
        pltpu.make_async_copy(signal_hbm, signal_ref, arrived.at[0]),
        pltpu.make_async_copy(basis_hbm, basis_ref, arrived.at[1]),
        pltpu.make_async_copy(table_hbm, table_ref, arrived.at[2]),
        pltpu.make_async_copy(transfer_hbm.at[:, pl.ds(0, levels)], transfer_ref, arrived.at[3]),
    ]
    for copy in copies:
        copy.start()
    for copy in copies[:2]:
        copy.wait()
    state = {}
    for box in range(0, boxes, 2):
        state[box] = project_pair(signal_ref, basis_ref, box, box + 1)
    for copy in copies[2:]:
        copy.wait()
    table = table_ref[...]
    for level in range(levels):
        bit = 1 << level
        blocks = [transfer_ref[box, level] for box in range(boxes)]
        matrices = level_matrices(blocks, [(box, box + bit) for box in state], table)
        done = {}
        for matrix, (box, pair) in zip(matrices, state.items()):
            both = dot(jnp.concatenate(split_rows(pair), axis=0), matrix)
            done[box] = both[:rhs] + both[rhs:]
        state = done
        if level + 1 < levels:
            state = {}
            for box in done:
                if box & (2 * bit):
                    continue
                other = box + 2 * bit
                state[box] = pick_low(done[box], half_roll(done[other]))
                state[box + bit] = pick_low(half_roll(done[box]), done[other])
    for box, pair in state.items():
        out_ref[box] = pair


def matrices_kernel(transfer_ref, table_ref, out_ref, *, first_level):
    boxes = transfer_ref.shape[0]
    half = boxes // 2
    table = table_ref[...]
    for level in range(out_ref.shape[0]):
        blocks = [transfer_ref[box, first_level + level] for box in range(boxes)]
        matrices = level_matrices(blocks, [(box, box + half) for box in range(half)], table)
        for box in range(half):
            out_ref[level, box] = matrices[box]


def crossed(own_ref, other_ref, matrices_ref, level, upper, box):
    own = own_ref[box]
    other = other_ref[box]
    rhs = own.shape[0]
    low = jnp.where(upper, other, own)
    high = jnp.where(upper, own, other)
    first = pick_low(low, half_roll(high))
    second = pick_low(half_roll(low), high)
    rows = jnp.concatenate(split_rows(first) + split_rows(second), axis=0)
    out = dot(rows, matrices_ref[level, box])
    return pick_low(out[:rhs] + out[rhs : 2 * rhs], out[2 * rhs : 3 * rhs] + out[3 * rhs :])


def device_index():
    return lax.axis_index("leaf") * lax.axis_size("sub") + lax.axis_index("sub")


def cross_kernel(index_ref, own_ref, other_ref, matrices_ref, out_ref, *, level):
    upper = (index_ref[0] >> level & 1) == 1
    for box in range(own_ref.shape[0]):
        out_ref[box] = crossed(own_ref, other_ref, matrices_ref, level, upper, box)


def final_kernel(
    index_ref, own_ref, other_ref, matrices_ref, basis_ref, center_ref, pair_ref, ring_ref, out_ref, *, level
):
    upper = (index_ref[0] >> level & 1) == 1
    odd = (index_ref[0] & 1) == 1
    half, rhs, width = own_ref.shape
    rank = width // 4
    edge = pair_ref.shape[1] // LEAF
    for box in range(half):
        pair = crossed(own_ref, other_ref, matrices_ref, level, upper, box)
        is_low = lanes_like(pair) < width // 2
        rows = []
        for part in (jnp.where(is_low, pair, 0.0), jnp.where(is_low, 0.0, pair)):
            rows += split_rows(part)
        right = []
        for place in (box, box + half):
            v = basis_ref[:, pl.ds(place * LEAF, LEAF)]
            right.append(jnp.concatenate([v[:rank], v[rank:]], axis=1))
            right.append(jnp.concatenate([-v[rank:], v[:rank]], axis=1))
        out = dot(jnp.concatenate(rows, axis=0), jnp.concatenate(right, axis=0))
        for k, place in enumerate((box, box + half)):
            far = out[2 * k * rhs : (2 * k + 1) * rhs] + out[(2 * k + 1) * rhs : (2 * k + 2) * rhs]
            total = center_ref[place] + jnp.concatenate([far[:, :LEAF], far[:, LEAF:]], axis=0)
            if place < edge:
                cols = pl.ds(place * LEAF, LEAF)
                total = total + jnp.where(odd, pair_ref[:, cols], ring_ref[:, cols])
            if place >= 2 * half - edge:
                cols = pl.ds((place - 2 * half + edge) * LEAF, LEAF)
                total = total + jnp.where(odd, ring_ref[:, cols], pair_ref[:, cols])
            out_ref[:, pl.ds(place * LEAF, LEAF)] = total


def near_kernel(
    index_ref, list_ref, signal_ref, pair_ref, ring_ref, blocks_ref, center_ref, to_pair_ref, to_ring_ref, window, sums
):
    odd = (index_ref[0] & 1) == 1
    channels = signal_ref.shape[0]
    rhs = channels // 2
    boxes = signal_ref.shape[1] // LEAF
    halo = pair_ref.shape[1] // LEAF
    edge = to_pair_ref.shape[1] // LEAF
    for box in range(halo):
        cols = pl.ds(box * LEAF, LEAF)
        window[box] = jnp.where(odd, pair_ref[:, cols], ring_ref[:, cols])
        window[halo + boxes + box] = jnp.where(odd, ring_ref[:, cols], pair_ref[:, cols])
    for box in range(boxes):
        window[halo + box] = signal_ref[:, pl.ds(box * LEAF, LEAF)]
    sums[...] = jnp.zeros_like(sums)
    for slot in range(blocks_ref.shape[0]):
        row = jnp.maximum(list_ref[0, slot], 0)
        col = list_ref[1, slot]
        col = jnp.where(col < 0, sums.shape[0] - 1, col)
        out = dot(window[row], blocks_ref[slot])
        real = out[:rhs, :LEAF] + out[rhs:, LEAF:]
        imag = out[rhs:, :LEAF] - out[:rhs, LEAF:]
        sums[col] = sums[col] + jnp.concatenate([real, imag], axis=0)
    for box in range(boxes):
        center_ref[box] = sums[edge + box]
    for box in range(edge):
        cols = pl.ds(box * LEAF, LEAF)
        before = sums[box]
        after = sums[edge + boxes + box]
        to_pair_ref[:, cols] = jnp.where(odd, before, after)
        to_ring_ref[:, cols] = jnp.where(odd, after, before)


VMEM = pl.BlockSpec(memory_space=pltpu.VMEM)
SMEM = pl.BlockSpec(memory_space=pltpu.SMEM)


def on_chip(kernel, outs, scalars, arrays, scratch=(), grant=16 << 20):
    single = len(outs) == 2 and not isinstance(outs[1], tuple)
    shapes = tuple(pltpu.VMEM(shape, kind) for shape, kind in ((outs,) if single else outs))
    call = pl.pallas_call(
        kernel,
        out_shape=shapes[0] if single else shapes,
        in_specs=[SMEM] * len(scalars) + [VMEM] * len(arrays),
        out_specs=VMEM if single else (VMEM,) * len(shapes),
        scratch_shapes=list(scratch),
        compiler_params=pltpu.CompilerParams(vmem_limit_bytes=grant),
    )
    return call(*scalars, *[pltpu.with_memory_space_constraint(x, pltpu.VMEM) for x in arrays])


def shards(signal, row_basis, transfer, column_basis, near_blocks, near_list):
    channels = signal.shape[0]
    rhs = channels // 2
    boxes, levels, rank, width = transfer.shape
    half = boxes // 2
    reach = boxes // 4
    local_levels = boxes.bit_length() - 1
    devices = lax.axis_size("leaf") * lax.axis_size("sub")
    index = device_index()
    index_word = index.astype(jnp.int32).reshape(1)
    odd = index & 1

    pairs = [(i, i ^ 1) for i in range(devices)]
    ring = [(i, (i + 1) % devices if i & 1 else (i - 1) % devices) for i in range(devices)]

    halo = 2 * reach * LEAF
    far_end = signal.shape[1] - halo
    to_pair = lax.dynamic_slice_in_dim(signal, jnp.where(odd == 1, 0, far_end), halo, 1)
    to_ring = lax.dynamic_slice_in_dim(signal, jnp.where(odd == 1, far_end, 0), halo, 1)
    from_pair = lax.ppermute(to_pair, AXES, pairs)
    from_ring = lax.ppermute(to_ring, AXES, ring)

    table = jnp.asarray(form_table(rank), BF16)
    state = ((half, rhs, width), F32)
    coeffs = pl.pallas_call(
        local_kernel,
        out_shape=pltpu.VMEM(*state),
        in_specs=[pl.BlockSpec(memory_space=pl.ANY)] * 4,
        out_specs=VMEM,
        scratch_shapes=[
            pltpu.VMEM(signal.shape, BF16),
            pltpu.VMEM(row_basis.shape, BF16),
            pltpu.VMEM((boxes, local_levels, rank, width), BF16),
            pltpu.VMEM(table.shape, BF16),
            pltpu.SemaphoreType.DMA((4,)),
        ],
        compiler_params=pltpu.CompilerParams(vmem_limit_bytes=16 << 20),
        name="local",
    )(*[pltpu.with_memory_space_constraint(x, pltpu.HBM) for x in (signal, row_basis, transfer, table)])
    cross_levels = levels - local_levels
    matrices = on_chip(
        functools.partial(matrices_kernel, first_level=local_levels),
        ((cross_levels, half, width, width), BF16),
        (),
        (transfer, table),
    )
    center, rim_pair, rim_ring = on_chip(
        near_kernel,
        (
            ((boxes, channels, LEAF), F32),
            ((channels, reach * LEAF), F32),
            ((channels, reach * LEAF), F32),
        ),
        (index_word, near_list.T),
        (signal, from_pair, from_ring, near_blocks),
        scratch=(
            pltpu.VMEM((boxes + 4 * reach, channels, LEAF), BF16),
            pltpu.VMEM((boxes + 2 * reach + 1, channels, LEAF), F32),
        ),
    )
    rim_from_pair = lax.ppermute(rim_pair, AXES, pairs)
    rim_from_ring = lax.ppermute(rim_ring, AXES, ring)

    for level in range(cross_levels):
        other = lax.ppermute(coeffs, AXES, [(i, i ^ 1 << level) for i in range(devices)])
        if level + 1 < cross_levels:
            coeffs = on_chip(
                functools.partial(cross_kernel, level=level), state, (index_word,), (coeffs, other, matrices)
            )
    return pl.pallas_call(
        functools.partial(final_kernel, level=cross_levels - 1),
        out_shape=jax.ShapeDtypeStruct((channels, boxes * LEAF), F32),
        in_specs=[SMEM] + [VMEM] * 7,
        out_specs=VMEM,
        compiler_params=pltpu.CompilerParams(vmem_limit_bytes=16 << 20),
        name="final",
    )(
        index_word,
        *[
            pltpu.with_memory_space_constraint(x, pltpu.VMEM)
            for x in (coeffs, other, matrices, column_basis, center, rim_from_pair, rim_from_ring)
        ],
    )


def solution(mesh):
    return jax.shard_map(
        shards,
        mesh=mesh,
        in_specs=(
            P(None, AXES),
            P(None, AXES),
            P(AXES, None, None, None),
            P(None, AXES),
            P(AXES, None, None),
            P(AXES, None),
        ),
        out_specs=P(None, AXES),
        check_vma=False,
    )
```

```python
import functools

import jax
import jax.numpy as jnp
import numpy as np
from jax import lax
from jax.experimental import pallas as pl
from jax.experimental.pallas import tpu as pltpu
from jax.sharding import PartitionSpec as P


LEAF = 128
AXES = ("leaf", "sub")
F32 = jnp.float32
BF16 = jnp.bfloat16


def lanes_like(x):
    return lax.broadcasted_iota(jnp.int32, x.shape, x.ndim - 1)


def dot(a, b):
    return lax.dot_general(a, b, (((1,), (0,)), ((), ())), preferred_element_type=F32)


def dot_t(a, b):
    return lax.dot_general(a, b, (((1,), (1,)), ((), ())), preferred_element_type=F32)


def half_roll(x):
    return pltpu.roll(x, x.shape[1] // 2, 1)


def pick_low(x, y):
    return jnp.where(lanes_like(x) < x.shape[1] // 2, x, y)


def split_rows(x):
    top = x.astype(BF16)
    rest = (x - top.astype(F32)).astype(BF16)
    return [top, rest]


def form_table(rank):
    width = 4 * rank
    table = np.zeros((2 * width, 4 * width), np.float32)
    unit = np.eye(rank, dtype=np.float32)
    for group in range(4):
        child, imag = divmod(group, 2)
        for box in range(2):
            for part in range(2):
                source = box * width + child * 2 * rank + (part ^ imag) * rank
                target = group * width + box * 2 * rank + part * rank
                sign = -1.0 if part and not imag else 1.0
                table[source : source + rank, target : target + rank] = sign * unit
    return table


def level_matrices(blocks, pairs, table):
    rows = [jnp.concatenate([blocks[first], blocks[second]], axis=1) for first, second in pairs]
    rank, width = rows[0].shape
    width //= 2
    out = dot(jnp.concatenate(rows, axis=0), table).astype(BF16)
    return [
        jnp.concatenate(
            [out[k * rank : (k + 1) * rank, g * width : (g + 1) * width] for g in range(4)], axis=0
        )
        for k in range(len(pairs))
    ]


def project_pair(signal_ref, basis_ref, first, second):
    rhs = signal_ref.shape[0] // 2
    rank = basis_ref.shape[0] // 2
    left = []
    right = []
    for box in (first, second):
        cols = pl.ds(box * LEAF, LEAF)
        x = signal_ref[:, cols]
        u = basis_ref[:, cols]
        left.append(jnp.concatenate([x[:rhs], x[rhs:]], axis=1))
        right.append(jnp.concatenate([u[:rank], u[rank:]], axis=1))
        right.append(jnp.concatenate([-u[rank:], u[:rank]], axis=1))
    out = dot_t(jnp.concatenate(left, axis=0), jnp.concatenate(right, axis=0))
    return pick_low(out[:rhs], out[rhs:])


def local_kernel(
    signal_hbm, basis_hbm, transfer_hbm, table_hbm, out_ref, signal_ref, basis_ref, transfer_ref, table_ref, arrived
):
    boxes, levels = transfer_ref.shape[:2]
    rhs = signal_ref.shape[0] // 2
    copies = [
        pltpu.make_async_copy(signal_hbm, signal_ref, arrived.at[0]),
        pltpu.make_async_copy(basis_hbm, basis_ref, arrived.at[1]),
        pltpu.make_async_copy(table_hbm, table_ref, arrived.at[2]),
        pltpu.make_async_copy(transfer_hbm.at[:, pl.ds(0, levels)], transfer_ref, arrived.at[3]),
    ]
    for copy in copies:
        copy.start()
    for copy in copies[:2]:
        copy.wait()
    state = {}
    for box in range(0, boxes, 2):
        state[box] = project_pair(signal_ref, basis_ref, box, box + 1)
    for copy in copies[2:]:
        copy.wait()
    table = table_ref[...]
    for level in range(levels):
        bit = 1 << level
        blocks = [transfer_ref[box, level] for box in range(boxes)]
        matrices = level_matrices(blocks, [(box, box + bit) for box in state], table)
        done = {}
        for matrix, (box, pair) in zip(matrices, state.items()):
            both = dot(jnp.concatenate(split_rows(pair), axis=0), matrix)
            done[box] = both[:rhs] + both[rhs:]
        state = done
        if level + 1 < levels:
            state = {}
            for box in done:
                if box & (2 * bit):
                    continue
                other = box + 2 * bit
                state[box] = pick_low(done[box], half_roll(done[other]))
                state[box + bit] = pick_low(half_roll(done[box]), done[other])
    for box, pair in state.items():
        out_ref[box] = pair


def matrices_kernel(transfer_ref, table_ref, out_ref, *, first_level):
    boxes = transfer_ref.shape[0]
    half = boxes // 2
    table = table_ref[...]
    for level in range(out_ref.shape[0]):
        blocks = [transfer_ref[box, first_level + level] for box in range(boxes)]
        matrices = level_matrices(blocks, [(box, box + half) for box in range(half)], table)
        for box in range(half):
            out_ref[level, box] = matrices[box]


CODE_STEPS = 256.0
CODE_MAX = 32767.0


def encode(parts):
    peak = jnp.abs(parts[0])
    for part in parts[1:]:
        peak = jnp.maximum(peak, jnp.abs(part))
    peak = jnp.maximum(jnp.max(peak, axis=1, keepdims=True), 1e-30)
    code = jnp.ceil(jnp.log2(peak) * CODE_STEPS) + 1.0
    gain = jnp.exp2(code * (-1.0 / CODE_STEPS)) * CODE_MAX
    coded = [jnp.round(part * gain) for part in parts] + [jnp.broadcast_to(code, parts[0].shape)]
    return [part.astype(jnp.int32).astype(jnp.int16) for part in coded]


def decode(ref):
    last = ref.shape[0] - 1
    gain = jnp.exp2(ref[last].astype(jnp.int32).astype(F32) * (1.0 / CODE_STEPS)) * (1.0 / CODE_MAX)
    return lambda box: ref[box].astype(jnp.int32).astype(F32) * gain


def crossed(own, other, matrix, upper):
    rhs = own.shape[0]
    low = jnp.where(upper, other, own)
    high = jnp.where(upper, own, other)
    first = pick_low(low, half_roll(high))
    second = pick_low(half_roll(low), high)
    rows = jnp.concatenate(split_rows(first) + split_rows(second), axis=0)
    out = dot(rows, matrix)
    return pick_low(out[:rhs] + out[rhs : 2 * rhs], out[2 * rhs : 3 * rhs] + out[3 * rhs :])


def device_index():
    return lax.axis_index("leaf") * lax.axis_size("sub") + lax.axis_index("sub")


def cross_kernel(index_ref, own_ref, other_ref, matrices_ref, out_ref, code_ref, *, level):
    upper = (index_ref[0] >> level & 1) == 1
    half = own_ref.shape[0]
    other = decode(other_ref) if level else lambda box: other_ref[box]
    outs = [crossed(own_ref[box], other(box), matrices_ref[level, box], upper) for box in range(half)]
    for box, part in enumerate(encode(outs)):
        code_ref[box] = part
    for box, part in enumerate(outs):
        out_ref[box] = part


def final_kernel(
    index_ref, own_ref, other_ref, matrices_ref, basis_ref, center_ref, pair_ref, ring_ref, out_ref, *, level
):
    upper = (index_ref[0] >> level & 1) == 1
    odd = (index_ref[0] & 1) == 1
    half, rhs, width = own_ref.shape
    rank = width // 4
    edge = pair_ref.shape[1] // LEAF
    other = decode(other_ref)
    for box in range(half):
        pair = crossed(own_ref[box], other(box), matrices_ref[level, box], upper)
        is_low = lanes_like(pair) < width // 2
        rows = []
        for part in (jnp.where(is_low, pair, 0.0), jnp.where(is_low, 0.0, pair)):
            rows += split_rows(part)
        right = []
        for place in (box, box + half):
            v = basis_ref[:, pl.ds(place * LEAF, LEAF)]
            right.append(jnp.concatenate([v[:rank], v[rank:]], axis=1))
            right.append(jnp.concatenate([-v[rank:], v[:rank]], axis=1))
        out = dot(jnp.concatenate(rows, axis=0), jnp.concatenate(right, axis=0))
        for k, place in enumerate((box, box + half)):
            far = out[2 * k * rhs : (2 * k + 1) * rhs] + out[(2 * k + 1) * rhs : (2 * k + 2) * rhs]
            total = center_ref[place] + jnp.concatenate([far[:, :LEAF], far[:, LEAF:]], axis=0)
            if place < edge:
                cols = pl.ds(place * LEAF, LEAF)
                total = total + jnp.where(odd, pair_ref[:, cols], ring_ref[:, cols])
            if place >= 2 * half - edge:
                cols = pl.ds((place - 2 * half + edge) * LEAF, LEAF)
                total = total + jnp.where(odd, ring_ref[:, cols], pair_ref[:, cols])
            out_ref[:, pl.ds(place * LEAF, LEAF)] = total


def near_kernel(
    index_ref, list_ref, signal_ref, pair_ref, ring_ref, blocks_ref, center_ref, to_pair_ref, to_ring_ref, window, sums
):
    odd = (index_ref[0] & 1) == 1
    channels = signal_ref.shape[0]
    rhs = channels // 2
    boxes = signal_ref.shape[1] // LEAF
    halo = pair_ref.shape[1] // LEAF
    edge = to_pair_ref.shape[1] // LEAF
    for box in range(halo):
        cols = pl.ds(box * LEAF, LEAF)
        window[box] = jnp.where(odd, pair_ref[:, cols], ring_ref[:, cols])
        window[halo + boxes + box] = jnp.where(odd, ring_ref[:, cols], pair_ref[:, cols])
    for box in range(boxes):
        window[halo + box] = signal_ref[:, pl.ds(box * LEAF, LEAF)]
    sums[...] = jnp.zeros_like(sums)
    for slot in range(blocks_ref.shape[0]):
        row = jnp.maximum(list_ref[0, slot], 0)
        col = list_ref[1, slot]
        col = jnp.where(col < 0, sums.shape[0] - 1, col)
        out = dot(window[row], blocks_ref[slot])
        real = out[:rhs, :LEAF] + out[rhs:, LEAF:]
        imag = out[rhs:, :LEAF] - out[:rhs, LEAF:]
        sums[col] = sums[col] + jnp.concatenate([real, imag], axis=0)
    for box in range(boxes):
        center_ref[box] = sums[edge + box]
    for box in range(edge):
        cols = pl.ds(box * LEAF, LEAF)
        before = sums[box]
        after = sums[edge + boxes + box]
        to_pair_ref[:, cols] = jnp.where(odd, before, after)
        to_ring_ref[:, cols] = jnp.where(odd, after, before)


VMEM = pl.BlockSpec(memory_space=pltpu.VMEM)
SMEM = pl.BlockSpec(memory_space=pltpu.SMEM)


def on_chip(kernel, outs, scalars, arrays, scratch=(), grant=16 << 20):
    single = len(outs) == 2 and not isinstance(outs[1], tuple)
    shapes = tuple(pltpu.VMEM(shape, kind) for shape, kind in ((outs,) if single else outs))
    call = pl.pallas_call(
        kernel,
        out_shape=shapes[0] if single else shapes,
        in_specs=[SMEM] * len(scalars) + [VMEM] * len(arrays),
        out_specs=VMEM if single else (VMEM,) * len(shapes),
        scratch_shapes=list(scratch),
        compiler_params=pltpu.CompilerParams(vmem_limit_bytes=grant),
    )
    return call(*scalars, *[pltpu.with_memory_space_constraint(x, pltpu.VMEM) for x in arrays])


def shards(signal, row_basis, transfer, column_basis, near_blocks, near_list):
    channels = signal.shape[0]
    rhs = channels // 2
    boxes, levels, rank, width = transfer.shape
    half = boxes // 2
    reach = boxes // 4
    local_levels = boxes.bit_length() - 1
    devices = lax.axis_size("leaf") * lax.axis_size("sub")
    index = device_index()
    index_word = index.astype(jnp.int32).reshape(1)
    odd = index & 1

    pairs = [(i, i ^ 1) for i in range(devices)]
    ring = [(i, (i + 1) % devices if i & 1 else (i - 1) % devices) for i in range(devices)]

    halo = 2 * reach * LEAF
    far_end = signal.shape[1] - halo
    to_pair = lax.dynamic_slice_in_dim(signal, jnp.where(odd == 1, 0, far_end), halo, 1)
    to_ring = lax.dynamic_slice_in_dim(signal, jnp.where(odd == 1, far_end, 0), halo, 1)
    from_pair = lax.ppermute(to_pair, AXES, pairs)
    from_ring = lax.ppermute(to_ring, AXES, ring)

    table = jnp.asarray(form_table(rank), BF16)
    state = ((half, rhs, width), F32)
    coeffs = pl.pallas_call(
        local_kernel,
        out_shape=pltpu.VMEM(*state),
        in_specs=[pl.BlockSpec(memory_space=pl.ANY)] * 4,
        out_specs=VMEM,
        scratch_shapes=[
            pltpu.VMEM(signal.shape, BF16),
            pltpu.VMEM(row_basis.shape, BF16),
            pltpu.VMEM((boxes, local_levels, rank, width), BF16),
            pltpu.VMEM(table.shape, BF16),
            pltpu.SemaphoreType.DMA((4,)),
        ],
        compiler_params=pltpu.CompilerParams(vmem_limit_bytes=16 << 20),
        name="local",
    )(*[pltpu.with_memory_space_constraint(x, pltpu.HBM) for x in (signal, row_basis, transfer, table)])
    cross_levels = levels - local_levels
    matrices = on_chip(
        functools.partial(matrices_kernel, first_level=local_levels),
        ((cross_levels, half, width, width), BF16),
        (),
        (transfer, table),
    )
    center, rim_pair, rim_ring = on_chip(
        near_kernel,
        (
            ((boxes, channels, LEAF), F32),
            ((channels, reach * LEAF), F32),
            ((channels, reach * LEAF), F32),
        ),
        (index_word, near_list.T),
        (signal, from_pair, from_ring, near_blocks),
        scratch=(
            pltpu.VMEM((boxes + 4 * reach, channels, LEAF), BF16),
            pltpu.VMEM((boxes + 2 * reach + 1, channels, LEAF), F32),
        ),
    )
    rim_from_pair = lax.ppermute(rim_pair, AXES, pairs)
    rim_from_ring = lax.ppermute(rim_ring, AXES, ring)

    sent = coeffs
    for level in range(cross_levels):
        other = lax.ppermute(sent, AXES, [(i, i ^ 1 << level) for i in range(devices)])
        if level + 1 < cross_levels:
            coeffs, sent = on_chip(
                functools.partial(cross_kernel, level=level),
                (state, ((half + 1, rhs, width), jnp.int16)),
                (index_word,),
                (coeffs, other, matrices),
            )
    return pl.pallas_call(
        functools.partial(final_kernel, level=cross_levels - 1),
        out_shape=jax.ShapeDtypeStruct((channels, boxes * LEAF), F32),
        in_specs=[SMEM] + [VMEM] * 7,
        out_specs=VMEM,
        compiler_params=pltpu.CompilerParams(vmem_limit_bytes=16 << 20),
        name="final",
    )(
        index_word,
        *[
            pltpu.with_memory_space_constraint(x, pltpu.VMEM)
            for x in (coeffs, other, matrices, column_basis, center, rim_from_pair, rim_from_ring)
        ],
    )


def solution(mesh):
    return jax.shard_map(
        shards,
        mesh=mesh,
        in_specs=(
            P(None, AXES),
            P(None, AXES),
            P(AXES, None, None, None),
            P(None, AXES),
            P(AXES, None, None),
            P(AXES, None),
        ),
        out_specs=P(None, AXES),
        check_vma=False,
    )
```

```python
import functools

import jax
import jax.numpy as jnp
from jax import lax
from jax.experimental import pallas as pl
from jax.experimental.pallas import tpu as pltpu
from jax.sharding import PartitionSpec as P


LEAF = 128
AXES = ("leaf", "sub")
F32 = jnp.float32
BF16 = jnp.bfloat16


def lanes_like(x):
    return lax.broadcasted_iota(jnp.int32, x.shape, x.ndim - 1)


def dot(a, b):
    return lax.dot_general(a, b, (((1,), (0,)), ((), ())), preferred_element_type=F32)


def dot_t(a, b):
    return lax.dot_general(a, b, (((1,), (1,)), ((), ())), preferred_element_type=F32)


def half_roll(x):
    return pltpu.roll(x, x.shape[1] // 2, 1)


def pick_low(x, y):
    return jnp.where(lanes_like(x) < x.shape[1] // 2, x, y)


def split_rows(x):
    top = x.astype(BF16)
    rest = (x - top.astype(F32)).astype(BF16)
    return [top, rest]


def form_table(rank, rows, columns):
    bit = rank.bit_length() - 1
    column = lax.broadcasted_iota(jnp.int32, (rows, columns), 1)
    row = lax.broadcasted_iota(jnp.int32, (rows, columns), 0)
    part = (column >> bit) & 1
    box = (column >> (bit + 1)) & 1
    imag = (column >> (bit + 2)) & 1
    child = column >> (bit + 3)
    source = (box << (bit + 2)) + (child << (bit + 1)) + ((part ^ imag) << bit) + (column & (rank - 1))
    value = jnp.where(part > imag, -1.0, 1.0)
    return jnp.where(row == source, value, 0.0).astype(BF16)


def level_matrices(blocks, pairs, table):
    rows = [jnp.concatenate([blocks[first], blocks[second]], axis=1) for first, second in pairs]
    rank, width = rows[0].shape
    width //= 2
    out = dot(jnp.concatenate(rows, axis=0), table).astype(BF16)
    return [
        jnp.concatenate(
            [out[k * rank : (k + 1) * rank, g * width : (g + 1) * width] for g in range(4)], axis=0
        )
        for k in range(len(pairs))
    ]


def project_pair(signal_ref, basis_ref, first, second):
    rhs = signal_ref.shape[0] // 2
    rank = basis_ref.shape[0] // 2
    left = []
    right = []
    for box in (first, second):
        cols = pl.ds(box * LEAF, LEAF)
        x = signal_ref[:, cols]
        u = basis_ref[:, cols]
        left.append(jnp.concatenate([x[:rhs], x[rhs:]], axis=1))
        right.append(jnp.concatenate([u[:rank], u[rank:]], axis=1))
        right.append(jnp.concatenate([-u[rank:], u[:rank]], axis=1))
    out = dot_t(jnp.concatenate(left, axis=0), jnp.concatenate(right, axis=0))
    return pick_low(out[:rhs], out[rhs:])


def local_kernel(
    index_ref,
    signal_hbm,
    basis_hbm,
    transfer_hbm,
    out_ref,
    signal_ref,
    transfer_ref,
    table_ref,
    to_pair_ref,
    to_ring_ref,
    basis_ref,
    arrived,
):
    boxes = transfer_ref.shape[0]
    levels = boxes.bit_length() - 1
    rhs = signal_ref.shape[0] // 2
    near_levels = pl.ds(0, levels)
    far_levels = pl.ds(levels, transfer_ref.shape[1] - levels)
    copies = [
        pltpu.make_async_copy(signal_hbm, signal_ref, arrived.at[0]),
        pltpu.make_async_copy(basis_hbm, basis_ref, arrived.at[1]),
        pltpu.make_async_copy(transfer_hbm.at[:, near_levels], transfer_ref.at[:, near_levels], arrived.at[2]),
        pltpu.make_async_copy(transfer_hbm.at[:, far_levels], transfer_ref.at[:, far_levels], arrived.at[3]),
    ]
    for copy in copies[:3]:
        copy.start()
    table_ref[...] = form_table(transfer_ref.shape[2], *table_ref.shape)
    for copy in copies[:2]:
        copy.wait()
    odd = (index_ref[0] & 1) == 1
    halo = to_pair_ref.shape[1]
    head = signal_ref[:, :halo]
    tail = signal_ref[:, signal_ref.shape[1] - halo :]
    to_pair_ref[...] = jnp.where(odd, head, tail)
    to_ring_ref[...] = jnp.where(odd, tail, head)
    state = {}
    for box in range(0, boxes, 2):
        state[box] = project_pair(signal_ref, basis_ref, box, box + 1)
    copies[2].wait()
    copies[3].start()
    table = table_ref[...]
    for level in range(levels):
        bit = 1 << level
        blocks = [transfer_ref[box, level] for box in range(boxes)]
        matrices = level_matrices(blocks, [(box, box + bit) for box in state], table)
        done = {}
        for matrix, (box, pair) in zip(matrices, state.items()):
            both = dot(jnp.concatenate(split_rows(pair), axis=0), matrix)
            done[box] = both[:rhs] + both[rhs:]
        state = done
        if level + 1 < levels:
            state = {}
            for box in done:
                if box & (2 * bit):
                    continue
                other = box + 2 * bit
                state[box] = pick_low(done[box], half_roll(done[other]))
                state[box + bit] = pick_low(half_roll(done[box]), done[other])
    for box, pair in state.items():
        out_ref[box] = pair
    copies[3].wait()


def matrices_kernel(transfer_ref, table_ref, own_ref, lent_ref, *, own_levels, lent_levels):
    boxes = transfer_ref.shape[0]
    half = boxes // 2
    table = table_ref[...]
    for levels, out_ref in ((lent_levels, lent_ref), (own_levels, own_ref)):
        for place, level in enumerate(levels):
            blocks = [transfer_ref[box, level] for box in range(boxes)]
            matrices = level_matrices(blocks, [(box, box + half) for box in range(half)], table)
            for box in range(half):
                out_ref[place, box] = matrices[box]


CODE_STEPS = 256.0
CODE_MAX = 32767.0


def encode(parts):
    peak = jnp.abs(parts[0])
    for part in parts[1:]:
        peak = jnp.maximum(peak, jnp.abs(part))
    peak = jnp.maximum(peak, 1e-30)
    code = jnp.ceil(jnp.log2(peak) * CODE_STEPS) + 1.0
    gain = jnp.exp2(code * (-1.0 / CODE_STEPS)) * CODE_MAX
    coded = [jnp.round(part * gain) for part in parts] + [code]
    return [part.astype(jnp.int32).astype(jnp.int16) for part in coded]


def decode(ref):
    last = ref.shape[0] - 1
    gain = jnp.exp2(ref[last].astype(jnp.int32).astype(F32) * (1.0 / CODE_STEPS)) * (1.0 / CODE_MAX)
    return lambda box: ref[box].astype(jnp.int32).astype(F32) * gain


def crossed(own, other, matrix, upper):
    rhs = own.shape[0]
    low = jnp.where(upper, other, own)
    high = jnp.where(upper, own, other)
    first = pick_low(low, half_roll(high))
    second = pick_low(half_roll(low), high)
    rows = jnp.concatenate(split_rows(first) + split_rows(second), axis=0)
    out = dot(rows, matrix)
    return pick_low(out[:rhs] + out[rhs : 2 * rhs], out[2 * rhs : 3 * rhs] + out[3 * rhs :])


def device_index():
    return lax.axis_index("leaf") * lax.axis_size("sub") + lax.axis_index("sub")


def cross_kernel(index_ref, own_ref, other_ref, matrices_ref, out_ref, code_ref, *, level, place):
    upper = (index_ref[0] >> level & 1) == 1
    half = own_ref.shape[0]
    other = decode(other_ref) if level else lambda box: other_ref[box]
    outs = [crossed(own_ref[box], other(box), matrices_ref[place, box], upper) for box in range(half)]
    for box, part in enumerate(encode(outs)):
        code_ref[box] = part
    for box, part in enumerate(outs):
        out_ref[box] = part


def final_kernel(
    index_ref, own_ref, other_ref, matrices_ref, basis_ref, center_ref, pair_ref, ring_ref, out_ref, *, level, place
):
    upper = (index_ref[0] >> level & 1) == 1
    odd = (index_ref[0] & 1) == 1
    half, rhs, width = own_ref.shape
    rank = width // 4
    edge = pair_ref.shape[0]
    other = decode(other_ref)
    from_ring = decode(ring_ref)
    for box in range(half):
        pair = crossed(own_ref[box], other(box), matrices_ref[place, box], upper)
        is_low = lanes_like(pair) < width // 2
        rows = []
        for part in (jnp.where(is_low, pair, 0.0), jnp.where(is_low, 0.0, pair)):
            rows += split_rows(part)
        right = []
        for spot in (box, box + half):
            v = basis_ref[:, pl.ds(spot * LEAF, LEAF)]
            right.append(jnp.concatenate([v[:rank], v[rank:]], axis=1))
            right.append(jnp.concatenate([-v[rank:], v[:rank]], axis=1))
        out = dot(jnp.concatenate(rows, axis=0), jnp.concatenate(right, axis=0))
        for k, spot in enumerate((box, box + half)):
            far = out[2 * k * rhs : (2 * k + 1) * rhs] + out[(2 * k + 1) * rhs : (2 * k + 2) * rhs]
            total = center_ref[spot] + jnp.concatenate([far[:, :LEAF], far[:, LEAF:]], axis=0)
            if spot < edge:
                total = total + jnp.where(odd, pair_ref[spot], from_ring(spot))
            if spot >= 2 * half - edge:
                rim = spot - 2 * half + edge
                total = total + jnp.where(odd, from_ring(rim), pair_ref[rim])
            out_ref[:, pl.ds(spot * LEAF, LEAF)] = total


def near_kernel(
    index_ref, list_ref, signal_ref, pair_ref, ring_ref, blocks_ref, center_ref, to_pair_ref, to_ring_ref, window, sums
):
    odd = (index_ref[0] & 1) == 1
    channels = signal_ref.shape[0]
    rhs = channels // 2
    boxes = signal_ref.shape[1] // LEAF
    halo = pair_ref.shape[1] // LEAF
    edge = to_pair_ref.shape[0]
    for box in range(halo):
        cols = pl.ds(box * LEAF, LEAF)
        window[box] = jnp.where(odd, pair_ref[:, cols], ring_ref[:, cols])
        window[halo + boxes + box] = jnp.where(odd, ring_ref[:, cols], pair_ref[:, cols])
    for box in range(boxes):
        window[halo + box] = signal_ref[:, pl.ds(box * LEAF, LEAF)]
    sums[...] = jnp.zeros_like(sums)
    for slot in range(blocks_ref.shape[0]):
        row = jnp.maximum(list_ref[0, slot], 0)
        col = list_ref[1, slot]
        col = jnp.where(col < 0, sums.shape[0] - 1, col)
        out = dot(window[row], blocks_ref[slot])
        real = out[:rhs, :LEAF] + out[rhs:, LEAF:]
        imag = out[rhs:, :LEAF] - out[:rhs, LEAF:]
        sums[col] = sums[col] + jnp.concatenate([real, imag], axis=0)
    for box in range(boxes):
        center_ref[box] = sums[edge + box]
    to_ring = []
    for box in range(edge):
        before = sums[box]
        after = sums[edge + boxes + box]
        to_pair_ref[box] = jnp.where(odd, before, after)
        to_ring.append(jnp.where(odd, after, before))
    for box, part in enumerate(encode(to_ring)):
        to_ring_ref[box] = part


VMEM = pl.BlockSpec(memory_space=pltpu.VMEM)
SMEM = pl.BlockSpec(memory_space=pltpu.SMEM)


def on_chip(kernel, outs, scalars, arrays, scratch=(), grant=16 << 20):
    single = len(outs) == 2 and not isinstance(outs[1], tuple)
    shapes = tuple(pltpu.VMEM(shape, kind) for shape, kind in ((outs,) if single else outs))
    call = pl.pallas_call(
        kernel,
        out_shape=shapes[0] if single else shapes,
        in_specs=[SMEM] * len(scalars) + [VMEM] * len(arrays),
        out_specs=VMEM if single else (VMEM,) * len(shapes),
        scratch_shapes=list(scratch),
        compiler_params=pltpu.CompilerParams(vmem_limit_bytes=grant),
    )
    return call(*scalars, *[pltpu.with_memory_space_constraint(x, pltpu.VMEM) for x in arrays])


def shards(signal, row_basis, transfer, column_basis, near_blocks, near_list):
    channels = signal.shape[0]
    rhs = channels // 2
    boxes, levels, _, width = transfer.shape
    half = boxes // 2
    reach = boxes // 4
    local_levels = boxes.bit_length() - 1
    devices = lax.axis_size("leaf") * lax.axis_size("sub")
    index = device_index()
    index_word = index.astype(jnp.int32).reshape(1)

    pairs = [(i, i ^ 1) for i in range(devices)]
    ring = [(i, (i + 1) % devices if i & 1 else (i - 1) % devices) for i in range(devices)]

    halo = 2 * reach * LEAF
    state = ((half, rhs, width), F32)
    coeffs, signal, transfer, table, to_pair, to_ring = pl.pallas_call(
        local_kernel,
        out_shape=(
            pltpu.VMEM(*state),
            pltpu.VMEM(signal.shape, BF16),
            pltpu.VMEM(transfer.shape, BF16),
            pltpu.VMEM((2 * width, 4 * width), BF16),
            pltpu.VMEM((channels, halo), BF16),
            pltpu.VMEM((channels, halo), BF16),
        ),
        in_specs=[SMEM] + [pl.BlockSpec(memory_space=pl.ANY)] * 3,
        out_specs=(VMEM,) * 6,
        scratch_shapes=[pltpu.VMEM(row_basis.shape, BF16), pltpu.SemaphoreType.DMA((4,))],
        compiler_params=pltpu.CompilerParams(vmem_limit_bytes=16 << 20),
        name="local",
    )(
        index_word,
        *[pltpu.with_memory_space_constraint(x, pltpu.HBM) for x in (signal, row_basis, transfer)],
    )
    from_pair = lax.ppermute(to_pair, AXES, pairs)
    from_ring = lax.ppermute(to_ring, AXES, ring)

    cross_levels = levels - local_levels
    crossing = crossings(cross_levels)
    lent = [bool(sum(crossing[level + 1 :]) & 1) for level in range(cross_levels)]
    own_levels = [level for level in range(cross_levels) if not lent[level]]
    lent_levels = [level for level in range(cross_levels) if lent[level]]
    own_matrices, to_lend = on_chip(
        functools.partial(
            matrices_kernel,
            own_levels=[local_levels + level for level in own_levels],
            lent_levels=[local_levels + level for level in lent_levels],
        ),
        (
            ((len(own_levels), half, width, width), BF16),
            ((len(lent_levels), half, width, width), BF16),
        ),
        (),
        (transfer, table),
    )
    lent_matrices = lax.ppermute(to_lend, AXES, pairs)
    center, rim_pair, rim_ring = on_chip(
        near_kernel,
        (
            ((boxes, channels, LEAF), F32),
            ((reach, channels, LEAF), F32),
            ((reach + 1, channels, LEAF), jnp.int16),
        ),
        (index_word, near_list.T),
        (signal, from_pair, from_ring, near_blocks),
        scratch=(
            pltpu.VMEM((boxes + 4 * reach, channels, LEAF), BF16),
            pltpu.VMEM((boxes + 2 * reach + 1, channels, LEAF), F32),
        ),
    )
    rim_from_pair = lax.ppermute(rim_pair, AXES, pairs)
    rim_from_ring = lax.ppermute(rim_ring, AXES, ring)

    sent = coeffs
    for level in range(cross_levels):
        flip = 1 << level | crossing[level]
        other = lax.ppermute(sent, AXES, [(i, i ^ flip) for i in range(devices)])
        if crossing[level]:
            coeffs = lax.ppermute(coeffs, AXES, pairs)
        matrices, place = (lent_matrices, lent_levels) if lent[level] else (own_matrices, own_levels)
        place = place.index(level)
        if level + 1 < cross_levels:
            coeffs, sent = on_chip(
                functools.partial(cross_kernel, level=level, place=place),
                (state, ((half + 1, rhs, width), jnp.int16)),
                (index_word,),
                (coeffs, other, matrices),
            )
    return pl.pallas_call(
        functools.partial(final_kernel, level=cross_levels - 1, place=place),
        out_shape=jax.ShapeDtypeStruct((channels, boxes * LEAF), F32),
        in_specs=[SMEM] + [VMEM] * 7,
        out_specs=VMEM,
        compiler_params=pltpu.CompilerParams(vmem_limit_bytes=16 << 20),
        name="final",
    )(
        index_word,
        *[
            pltpu.with_memory_space_constraint(x, pltpu.VMEM)
            for x in (coeffs, other, matrices, column_basis, center, rim_from_pair, rim_from_ring)
        ],
    )


def crossings(levels):
    return [int(level - levels in CROSSED) for level in range(levels)]


CROSSED = (-3, -1)


def solution(mesh):
    return jax.shard_map(
        shards,
        mesh=mesh,
        in_specs=(
            P(None, AXES),
            P(None, AXES),
            P(AXES, None, None, None),
            P(None, AXES),
            P(AXES, None, None),
            P(AXES, None),
        ),
        out_specs=P(None, AXES),
        check_vma=False,
    )
```

```python
import functools

import jax
import jax.numpy as jnp
from jax import lax
from jax.experimental import pallas as pl
from jax.experimental.pallas import tpu as pltpu
from jax.sharding import PartitionSpec as P


LEAF = 128
AXES = ("leaf", "sub")
F32 = jnp.float32
BF16 = jnp.bfloat16


def lanes_like(x):
    return lax.broadcasted_iota(jnp.int32, x.shape, x.ndim - 1)


def dot(a, b):
    return lax.dot_general(a, b, (((1,), (0,)), ((), ())), preferred_element_type=F32)


def dot_t(a, b):
    return lax.dot_general(a, b, (((1,), (1,)), ((), ())), preferred_element_type=F32)


def half_roll(x):
    return pltpu.roll(x, x.shape[1] // 2, 1)


def pick_low(x, y):
    return jnp.where(lanes_like(x) < x.shape[1] // 2, x, y)


def split_rows(x):
    top = x.astype(BF16)
    rest = (x - top.astype(F32)).astype(BF16)
    return [top, rest]


def form_table(rank, rows, columns):
    bit = rank.bit_length() - 1
    column = lax.broadcasted_iota(jnp.int32, (rows, columns), 1)
    row = lax.broadcasted_iota(jnp.int32, (rows, columns), 0)
    part = (column >> bit) & 1
    box = (column >> (bit + 1)) & 1
    imag = (column >> (bit + 2)) & 1
    child = column >> (bit + 3)
    source = (box << (bit + 2)) + (child << (bit + 1)) + ((part ^ imag) << bit) + (column & (rank - 1))
    value = jnp.where(part > imag, -1.0, 1.0)
    return jnp.where(row == source, value, 0.0).astype(BF16)


def level_matrices(blocks, pairs, table):
    rows = [jnp.concatenate([blocks[first], blocks[second]], axis=1) for first, second in pairs]
    rank, width = rows[0].shape
    width //= 2
    out = dot(jnp.concatenate(rows, axis=0), table).astype(BF16)
    return [
        jnp.concatenate(
            [out[k * rank : (k + 1) * rank, g * width : (g + 1) * width] for g in range(4)], axis=0
        )
        for k in range(len(pairs))
    ]


def project_pair(signal_ref, basis_ref, first, second):
    rhs = signal_ref.shape[0] // 2
    rank = basis_ref.shape[0] // 2
    left = []
    right = []
    for box in (first, second):
        cols = pl.ds(box * LEAF, LEAF)
        x = signal_ref[:, cols]
        u = basis_ref[:, cols]
        left.append(jnp.concatenate([x[:rhs], x[rhs:]], axis=1))
        right.append(jnp.concatenate([u[:rank], u[rank:]], axis=1))
        right.append(jnp.concatenate([-u[rank:], u[:rank]], axis=1))
    out = dot_t(jnp.concatenate(left, axis=0), jnp.concatenate(right, axis=0))
    return pick_low(out[:rhs], out[rhs:])


def local_kernel(
    index_ref,
    signal_hbm,
    basis_hbm,
    transfer_hbm,
    list_hbm,
    out_ref,
    signal_ref,
    transfer_ref,
    table_ref,
    to_pair_ref,
    to_ring_ref,
    list_ref,
    basis_ref,
    arrived,
):
    boxes = transfer_ref.shape[0]
    levels = boxes.bit_length() - 1
    rhs = signal_ref.shape[0] // 2
    near_levels = pl.ds(0, levels)
    far_levels = pl.ds(levels, transfer_ref.shape[1] - levels)
    copies = [
        pltpu.make_async_copy(signal_hbm, signal_ref, arrived.at[0]),
        pltpu.make_async_copy(basis_hbm, basis_ref, arrived.at[1]),
        pltpu.make_async_copy(transfer_hbm.at[:, near_levels], transfer_ref.at[:, near_levels], arrived.at[2]),
        pltpu.make_async_copy(transfer_hbm.at[:, far_levels], transfer_ref.at[:, far_levels], arrived.at[3]),
        pltpu.make_async_copy(list_hbm, list_ref, arrived.at[4]),
    ]
    for copy in copies[:3]:
        copy.start()
    table_ref[...] = form_table(transfer_ref.shape[2], *table_ref.shape)
    for copy in copies[:2]:
        copy.wait()
    odd = (index_ref[0] & 1) == 1
    halo = to_pair_ref.shape[1]
    head = signal_ref[:, :halo]
    tail = signal_ref[:, signal_ref.shape[1] - halo :]
    to_pair_ref[...] = jnp.where(odd, head, tail)
    to_ring_ref[...] = jnp.where(odd, tail, head)
    state = {}
    for box in range(0, boxes, 2):
        state[box] = project_pair(signal_ref, basis_ref, box, box + 1)
    copies[2].wait()
    for copy in copies[3:]:
        copy.start()
    table = table_ref[...]
    for level in range(levels):
        bit = 1 << level
        blocks = [transfer_ref[box, level] for box in range(boxes)]
        matrices = level_matrices(blocks, [(box, box + bit) for box in state], table)
        done = {}
        for matrix, (box, pair) in zip(matrices, state.items()):
            both = dot(jnp.concatenate(split_rows(pair), axis=0), matrix)
            done[box] = both[:rhs] + both[rhs:]
        state = done
        if level + 1 < levels:
            state = {}
            for box in done:
                if box & (2 * bit):
                    continue
                other = box + 2 * bit
                state[box] = pick_low(done[box], half_roll(done[other]))
                state[box + bit] = pick_low(half_roll(done[box]), done[other])
    for box, pair in state.items():
        out_ref[box] = pair
    for copy in copies[3:]:
        copy.wait()


def matrices_kernel(transfer_ref, table_ref, own_ref, lent_ref, *, own_levels, lent_levels):
    boxes = transfer_ref.shape[0]
    half = boxes // 2
    table = table_ref[...]
    for levels, out_ref in ((lent_levels, lent_ref), (own_levels, own_ref)):
        for place, level in enumerate(levels):
            blocks = [transfer_ref[box, level] for box in range(boxes)]
            matrices = level_matrices(blocks, [(box, box + half) for box in range(half)], table)
            for box in range(half):
                out_ref[place, box] = matrices[box]


CODE_STEPS = 256.0
CODE_MAX = 32767.0


def encode(parts):
    peak = jnp.abs(parts[0])
    for part in parts[1:]:
        peak = jnp.maximum(peak, jnp.abs(part))
    peak = jnp.maximum(peak, 1e-30)
    code = jnp.ceil(jnp.log2(peak) * CODE_STEPS) + 1.0
    gain = jnp.exp2(code * (-1.0 / CODE_STEPS)) * CODE_MAX
    coded = [jnp.round(part * gain) for part in parts] + [code]
    return [part.astype(jnp.int32).astype(jnp.int16) for part in coded]


def decode(ref):
    last = ref.shape[0] - 1
    gain = jnp.exp2(ref[last].astype(jnp.int32).astype(F32) * (1.0 / CODE_STEPS)) * (1.0 / CODE_MAX)
    return lambda box: ref[box].astype(jnp.int32).astype(F32) * gain


def crossed(own, other, matrix, upper):
    rhs = own.shape[0]
    low = jnp.where(upper, other, own)
    high = jnp.where(upper, own, other)
    first = pick_low(low, half_roll(high))
    second = pick_low(half_roll(low), high)
    rows = jnp.concatenate(split_rows(first) + split_rows(second), axis=0)
    out = dot(rows, matrix)
    return pick_low(out[:rhs] + out[rhs : 2 * rhs], out[2 * rhs : 3 * rhs] + out[3 * rhs :])


def device_index():
    return lax.axis_index("leaf") * lax.axis_size("sub") + lax.axis_index("sub")


def cross_kernel(index_ref, own_ref, other_ref, matrices_ref, out_ref, code_ref, *, level, place):
    upper = (index_ref[0] >> level & 1) == 1
    half = own_ref.shape[0]
    other = decode(other_ref) if level else lambda box: other_ref[box]
    outs = [crossed(own_ref[box], other(box), matrices_ref[place, box], upper) for box in range(half)]
    for box, part in enumerate(encode(outs)):
        code_ref[box] = part
    for box, part in enumerate(outs):
        out_ref[box] = part


def final_kernel(
    index_ref, own_ref, other_ref, matrices_ref, basis_ref, center_ref, pair_ref, ring_ref, out_ref, *, level, place
):
    upper = (index_ref[0] >> level & 1) == 1
    odd = (index_ref[0] & 1) == 1
    half, rhs, width = own_ref.shape
    rank = width // 4
    edge = pair_ref.shape[0]
    other = decode(other_ref)
    from_ring = decode(ring_ref)
    for box in range(half):
        pair = crossed(own_ref[box], other(box), matrices_ref[place, box], upper)
        is_low = lanes_like(pair) < width // 2
        rows = []
        for part in (jnp.where(is_low, pair, 0.0), jnp.where(is_low, 0.0, pair)):
            rows += split_rows(part)
        right = []
        for spot in (box, box + half):
            v = basis_ref[:, pl.ds(spot * LEAF, LEAF)]
            right.append(jnp.concatenate([v[:rank], v[rank:]], axis=1))
            right.append(jnp.concatenate([-v[rank:], v[:rank]], axis=1))
        out = dot(jnp.concatenate(rows, axis=0), jnp.concatenate(right, axis=0))
        for k, spot in enumerate((box, box + half)):
            far = out[2 * k * rhs : (2 * k + 1) * rhs] + out[(2 * k + 1) * rhs : (2 * k + 2) * rhs]
            total = center_ref[spot] + jnp.concatenate([far[:, :LEAF], far[:, LEAF:]], axis=0)
            if spot < edge:
                total = total + jnp.where(odd, pair_ref[spot], from_ring(spot))
            if spot >= 2 * half - edge:
                rim = spot - 2 * half + edge
                total = total + jnp.where(odd, from_ring(rim), pair_ref[rim])
            out_ref[:, pl.ds(spot * LEAF, LEAF)] = total


def near_kernel(
    index_ref, list_ref, signal_ref, pair_ref, ring_ref, blocks_ref, center_ref, to_pair_ref, to_ring_ref, window, sums
):
    odd = (index_ref[0] & 1) == 1
    channels = signal_ref.shape[0]
    rhs = channels // 2
    boxes = signal_ref.shape[1] // LEAF
    halo = pair_ref.shape[1] // LEAF
    edge = to_pair_ref.shape[0]
    for box in range(halo):
        cols = pl.ds(box * LEAF, LEAF)
        window[box] = jnp.where(odd, pair_ref[:, cols], ring_ref[:, cols])
        window[halo + boxes + box] = jnp.where(odd, ring_ref[:, cols], pair_ref[:, cols])
    for box in range(boxes):
        window[halo + box] = signal_ref[:, pl.ds(box * LEAF, LEAF)]
    sums[...] = jnp.zeros_like(sums)
    for slot in range(blocks_ref.shape[0]):
        row = jnp.maximum(list_ref[0, slot], 0)
        col = list_ref[1, slot]
        col = jnp.where(col < 0, sums.shape[0] - 1, col)
        out = dot(window[row], blocks_ref[slot])
        real = out[:rhs, :LEAF] + out[rhs:, LEAF:]
        imag = out[rhs:, :LEAF] - out[:rhs, LEAF:]
        sums[col] = sums[col] + jnp.concatenate([real, imag], axis=0)
    for box in range(boxes):
        center_ref[box] = sums[edge + box]
    to_ring = []
    for box in range(edge):
        before = sums[box]
        after = sums[edge + boxes + box]
        to_pair_ref[box] = jnp.where(odd, before, after)
        to_ring.append(jnp.where(odd, after, before))
    for box, part in enumerate(encode(to_ring)):
        to_ring_ref[box] = part


VMEM = pl.BlockSpec(memory_space=pltpu.VMEM)
SMEM = pl.BlockSpec(memory_space=pltpu.SMEM)


def on_chip(kernel, outs, scalars, arrays, scratch=(), grant=16 << 20):
    single = len(outs) == 2 and not isinstance(outs[1], tuple)
    shapes = tuple(pltpu.VMEM(shape, kind) for shape, kind in ((outs,) if single else outs))
    call = pl.pallas_call(
        kernel,
        out_shape=shapes[0] if single else shapes,
        in_specs=[SMEM] * len(scalars) + [VMEM] * len(arrays),
        out_specs=VMEM if single else (VMEM,) * len(shapes),
        scratch_shapes=list(scratch),
        compiler_params=pltpu.CompilerParams(vmem_limit_bytes=grant),
    )
    return call(*scalars, *[pltpu.with_memory_space_constraint(x, pltpu.VMEM) for x in arrays])


def shards(signal, row_basis, transfer, column_basis, near_blocks, near_list):
    channels = signal.shape[0]
    rhs = channels // 2
    boxes, levels, _, width = transfer.shape
    half = boxes // 2
    reach = boxes // 4
    local_levels = boxes.bit_length() - 1
    devices = lax.axis_size("leaf") * lax.axis_size("sub")
    index = device_index()
    index_word = index.astype(jnp.int32).reshape(1)

    pairs = [(i, i ^ 1) for i in range(devices)]
    ring = [(i, (i + 1) % devices if i & 1 else (i - 1) % devices) for i in range(devices)]

    halo = 2 * reach * LEAF
    state = ((half, rhs, width), F32)
    coeffs, signal, transfer, table, to_pair, to_ring, slots = pl.pallas_call(
        local_kernel,
        out_shape=(
            pltpu.VMEM(*state),
            pltpu.VMEM(signal.shape, BF16),
            pltpu.VMEM(transfer.shape, BF16),
            pltpu.VMEM((2 * width, 4 * width), BF16),
            pltpu.VMEM((channels, halo), BF16),
            pltpu.VMEM((channels, halo), BF16),
            pltpu.SMEM(near_list.shape[::-1], jnp.int32),
        ),
        in_specs=[SMEM] + [pl.BlockSpec(memory_space=pl.ANY)] * 4,
        out_specs=(VMEM,) * 6 + (SMEM,),
        scratch_shapes=[pltpu.VMEM(row_basis.shape, BF16), pltpu.SemaphoreType.DMA((5,))],
        compiler_params=pltpu.CompilerParams(vmem_limit_bytes=16 << 20),
        name="local",
    )(
        index_word,
        *[pltpu.with_memory_space_constraint(x, pltpu.HBM) for x in (signal, row_basis, transfer, near_list.T)],
    )
    from_pair = lax.ppermute(to_pair, AXES, pairs)
    from_ring = lax.ppermute(to_ring, AXES, ring)

    cross_levels = levels - local_levels
    crossing = crossings(cross_levels)
    lent = [bool(sum(crossing[level + 1 :]) & 1) for level in range(cross_levels)]
    own_levels = [level for level in range(cross_levels) if not lent[level]]
    lent_levels = [level for level in range(cross_levels) if lent[level]]
    own_matrices, to_lend = on_chip(
        functools.partial(
            matrices_kernel,
            own_levels=[local_levels + level for level in own_levels],
            lent_levels=[local_levels + level for level in lent_levels],
        ),
        (
            ((len(own_levels), half, width, width), BF16),
            ((len(lent_levels), half, width, width), BF16),
        ),
        (),
        (transfer, table),
    )
    lent_matrices = lax.ppermute(to_lend, AXES, pairs)
    center, rim_pair, rim_ring = on_chip(
        near_kernel,
        (
            ((boxes, channels, LEAF), F32),
            ((reach, channels, LEAF), F32),
            ((reach + 1, channels, LEAF), jnp.int16),
        ),
        (index_word, pltpu.with_memory_space_constraint(slots, pltpu.SMEM)),
        (signal, from_pair, from_ring, near_blocks),
        scratch=(
            pltpu.VMEM((boxes + 4 * reach, channels, LEAF), BF16),
            pltpu.VMEM((boxes + 2 * reach + 1, channels, LEAF), F32),
        ),
    )
    rim_from_pair = lax.ppermute(rim_pair, AXES, pairs)
    rim_from_ring = lax.ppermute(rim_ring, AXES, ring)

    sent = coeffs
    for level in range(cross_levels):
        flip = 1 << level | crossing[level]
        other = lax.ppermute(sent, AXES, [(i, i ^ flip) for i in range(devices)])
        if crossing[level]:
            coeffs = lax.ppermute(coeffs, AXES, pairs)
        matrices, place = (lent_matrices, lent_levels) if lent[level] else (own_matrices, own_levels)
        place = place.index(level)
        if level + 1 < cross_levels:
            coeffs, sent = on_chip(
                functools.partial(cross_kernel, level=level, place=place),
                (state, ((half + 1, rhs, width), jnp.int16)),
                (index_word,),
                (coeffs, other, matrices),
            )
    return pl.pallas_call(
        functools.partial(final_kernel, level=cross_levels - 1, place=place),
        out_shape=jax.ShapeDtypeStruct((channels, boxes * LEAF), F32),
        in_specs=[SMEM] + [VMEM] * 7,
        out_specs=VMEM,
        compiler_params=pltpu.CompilerParams(vmem_limit_bytes=16 << 20),
        name="final",
    )(
        index_word,
        *[
            pltpu.with_memory_space_constraint(x, pltpu.VMEM)
            for x in (coeffs, other, matrices, column_basis, center, rim_from_pair, rim_from_ring)
        ],
    )


def crossings(levels):
    return [int(level - levels in CROSSED) for level in range(levels)]


CROSSED = (-4, -3, -2, -1)


def solution(mesh):
    return jax.shard_map(
        shards,
        mesh=mesh,
        in_specs=(
            P(None, AXES),
            P(None, AXES),
            P(AXES, None, None, None),
            P(None, AXES),
            P(AXES, None, None),
            P(AXES, None),
        ),
        out_specs=P(None, AXES),
        check_vma=False,
    )
```
